128 devices in a mesh: blocks: 64 (over x, z, y), cross: 2 (over core).
Axes of the slice: x: 4, y: 4, z: 4, core: 2. Of those that a mesh axis runs over, the one named last changes fastest.
Arguments:
- f_home: float32 [4096, 19, 512], P(('blocks', 'cross')), may hold values from -0.5 to 1.5
- levels: int32 [4096], P(('blocks', 'cross')), may hold values from 0 to 1, as said below
- plan: int32 [4096], P(('blocks', 'cross')), may hold values from 0 to 4095, as said below
Outputs:
- f_owner: float32 [4096, 19, 512], P(('blocks', 'cross'))
The draws below stay inside these ranges and needn't reach their ends.
Inputs may be any that keep to these rules, and one draw needn't show every extreme that they name: `levels`: exactly a quarter of the patches, 8 times the number of devices, have level 1. plan is a permutation of the patch numbers. Of the patches in the slots of one device of f_home, at most 2 have owner slots on one device, and in every draw some device sends exactly 2 to one owner; every device's owner slots receive exactly 8 patches of level 1.
All inputs are finite; a program needn't handle non-finite values.
Results may differ from the reference program's by a relative error of at most 0.0001.
Values sent between devices are 32-bit elements; how exact they have to be, the bound alone decides.
A program may use at most 256 MiB of HBM per device.

```python
import jax
import jax.numpy as jnp
from jax import lax

FLOW_PATCHES = 1
SPAN_PATCHES = 4
DEPTH_PATCHES = 8
EDGE = 8
STEPS = 2
CELLS = 512
PATCH_DEV = 32
FINE_DEV = 8
PATCHES = 4096
N_BLOCKS = 64
N_CROSS = 2
DEVICES = 128


VELOCITIES = ((0, 0, 0), (1, 0, 0), (-1, 0, 0), (0, 1, 0), (0, -1, 0), (0, 0, 1), (0, 0, -1), (1, 1, 0), (-1, -1, 0), (1, -1, 0), (-1, 1, 0), (1, 0, 1), (-1, 0, -1), (1, 0, -1), (-1, 0, 1), (0, 1, 1), (0, -1, -1), (0, 1, -1), (0, -1, 1))


WEIGHTS = (1.0 / 3.0,) + (1.0 / 18.0,) * 6 + (1.0 / 36.0,) * 12


def wake_layout(key):
    key_tie = jax.random.fold_in(key, 7)
    key_owner = jax.random.fold_in(key, 8)
    key_slot = jax.random.fold_in(key, 9)
    key_jitter = jax.random.fold_in(key, 10)
    ident = jnp.arange(PATCHES, dtype=jnp.int32)
    home = ident // PATCH_DEV
    local_id = ident % PATCH_DEV
    flow_x = home // N_CROSS * FLOW_PATCHES + local_id // (SPAN_PATCHES * DEPTH_PATCHES)
    span_y = home % N_CROSS * SPAN_PATCHES + local_id // DEPTH_PATCHES % SPAN_PATCHES
    total_x = FLOW_PATCHES * N_BLOCKS
    total_y = SPAN_PATCHES * N_CROSS
    behind = flow_x - total_x // 8
    lateral = jnp.abs(2 * span_y + 1 - total_y)
    jitter = jax.random.randint(key_jitter, (PATCHES,), 0, 3 * total_x)
    score = jnp.where(behind >= 0, 8 * total_x * total_y, 0) - lateral * total_x - jnp.abs(behind - total_x // 4) * total_y + jitter
    ties = jax.random.permutation(key_tie, PATCHES).astype(jnp.int32)
    order = jnp.argsort(-(score * PATCHES + ties))
    fine_mask = jnp.zeros((PATCHES,), jnp.int32).at[order[:PATCHES // 4]].set(1)
    fine_rank = jnp.cumsum(fine_mask) - 1
    coarse_rank = jnp.cumsum(1 - fine_mask) - 1
    home_fine = jnp.sum(fine_mask.reshape(DEVICES, PATCH_DEV), axis=1)
    home_coarse = PATCH_DEV - home_fine
    fine_before = jnp.cumsum(home_fine) - home_fine
    coarse_before = jnp.arange(DEVICES, dtype=jnp.int32) * PATCH_DEV - fine_before
    chosen = jnp.argmax(jnp.where(home_coarse > 0, home_fine, -1))
    offset = (fine_before[chosen] - coarse_before[chosen] - home_coarse[chosen] + 1) % DEVICES
    coarse_total = PATCHES - PATCHES // 4
    coarse_index = (coarse_rank + offset) % coarse_total
    owner_pos = jnp.where(fine_mask == 1, fine_rank % DEVICES, coarse_index % DEVICES)
    slot_rank = jnp.where(fine_mask == 1, fine_rank // DEVICES, FINE_DEV + coarse_index // DEVICES)
    relabel = jax.random.permutation(key_owner, DEVICES).astype(jnp.int32)
    slot_scores = jax.random.randint(key_slot, (DEVICES, PATCH_DEV), 0, 1 << 20) * PATCH_DEV + jnp.arange(PATCH_DEV, dtype=jnp.int32)[None, :]
    shuffle = jnp.argsort(slot_scores, axis=1).astype(jnp.int32)
    plan = relabel[owner_pos] * PATCH_DEV + shuffle[owner_pos, slot_rank]
    return (fine_mask.astype(jnp.int32), plan.astype(jnp.int32))


def draw_levels(key, part):
    return wake_layout(key)[0]


def draw_plan(key, part):
    return wake_layout(key)[1]


def draw_f_home(key, part):
    key_density = jax.random.fold_in(key, 21)
    key_velocity = jax.random.fold_in(key, 22)
    key_jitter = jax.random.fold_in(key, 23)
    density = 1.0 + 0.05 * jax.random.truncated_normal(key_density, -3.0, 3.0, (PATCHES, CELLS), jnp.float32)
    velocity = 0.03 * jax.random.truncated_normal(key_velocity, -3.0, 3.0, (3, PATCHES, CELLS), jnp.float32)
    velocity = velocity.at[0].add(0.05)
    jitter = jax.random.truncated_normal(key_jitter, -3.0, 3.0, (PATCHES, 19, CELLS), jnp.float32)
    speed_sq = velocity[0] * velocity[0] + velocity[1] * velocity[1] + velocity[2] * velocity[2]
    columns = []
    for speed in range(19):
        step_x, step_y, step_z = VELOCITIES[speed]
        along = step_x * velocity[0] + step_y * velocity[1] + step_z * velocity[2]
        columns.append(WEIGHTS[speed] * (density * (1.0 + 3.0 * along + 4.5 * along * along - 1.5 * speed_sq) + 0.3 * jitter[:, speed]))
    return jnp.stack(columns, axis=1).astype(jnp.float32)


def block_scale(rng, shape, split, low, top_value):
    loudness = 1.0
    for dim, shards_of in split:
        steps = jax.random.uniform(jax.random.fold_in(jax.random.fold_in(rng, 6), dim), (shards_of,), jnp.float32, low / len(split), top_value / len(split))
        loudness = loudness * jnp.repeat(jnp.exp(steps), shape[dim] // shards_of).reshape((-1,) + (1,) * (len(shape) - 1 - dim))
    return loudness


def setup_inputs(seed: int = 0) -> dict:
    seeds = jax.random.split(jax.random.key(seed), 4)
    f_home = draw_f_home(jax.random.fold_in(seeds[3], 71), 0)
    levels = draw_levels(jax.random.fold_in(seeds[3], 71), 0)
    plan = draw_plan(jax.random.fold_in(seeds[3], 71), 0)
    return dict(f_home=f_home, levels=levels, plan=plan)


VELOCITIES = ((0, 0, 0), (1, 0, 0), (-1, 0, 0), (0, 1, 0), (0, -1, 0), (0, 0, 1), (0, 0, -1), (1, 1, 0), (-1, -1, 0), (1, -1, 0), (-1, 1, 0), (1, 0, 1), (-1, 0, -1), (1, 0, -1), (-1, 0, 1), (0, 1, 1), (0, -1, -1), (0, 1, -1), (0, -1, 1))
WEIGHTS = (1.0 / 3.0,) + (1.0 / 18.0,) * 6 + (1.0 / 36.0,) * 12
FACE_SPEEDS = ((2, 8, 10, 12, 14), (1, 7, 9, 11, 13), (4, 8, 9, 16, 18), (3, 7, 10, 15, 17), (6, 12, 13, 16, 17), (5, 11, 14, 15, 18))
TAU_COARSE = 0.55
TAU_FINE = 2.0 * TAU_COARSE - 0.5
RESCALE = TAU_FINE / (2.0 * TAU_COARSE)
INFLOW = 0.08


def moments(field):
    density = jnp.sum(field, axis=1)
    velocity = []
    for axis_id in range(3):
        forward = [speed for speed in range(19) if VELOCITIES[speed][axis_id] == 1]
        backward = [speed for speed in range(19) if VELOCITIES[speed][axis_id] == -1]
        velocity.append((jnp.sum(field[:, forward], axis=1) - jnp.sum(field[:, backward], axis=1)) / density)
    return density, velocity


def equilibrium(density, velocity, speeds):
    speed_sq = velocity[0] * velocity[0] + velocity[1] * velocity[1] + velocity[2] * velocity[2]
    columns = []
    for speed in speeds:
        step_x, step_y, step_z = VELOCITIES[speed]
        along = step_x * velocity[0] + step_y * velocity[1] + step_z * velocity[2]
        columns.append(WEIGHTS[speed] * density * (1.0 + 3.0 * along + 4.5 * along * along - 1.5 * speed_sq))
    return jnp.stack(columns, axis=1)


def collide(field, relax_rate):
    density, velocity = moments(field)
    balance = equilibrium(density, velocity, range(19))
    relaxed = field + relax_rate[:, None, None, None, None] * (balance - field)
    return relaxed, balance, density, velocity


def layer(field, face_id):
    layer_at = 0 if face_id % 2 == 0 else field.shape[-1] - 1
    return jnp.take(field, layer_at, axis=2 + face_id // 2)


def face_payload(relaxed, balance, send_scale):
    eq_faces = jnp.stack([layer(balance[:, list(FACE_SPEEDS[face_id])], face_id) for face_id in range(6)], axis=1)
    out_faces = jnp.stack([layer(relaxed[:, list(FACE_SPEEDS[face_id])], face_id) for face_id in range(6)], axis=1)
    return eq_faces, send_scale[:, None, None, None, None] * (out_faces - eq_faces)


def inflow_column(speeds):
    values = []
    for speed in speeds:
        along = VELOCITIES[speed][0] * INFLOW
        values.append(WEIGHTS[speed] * (1.0 + 3.0 * along + 4.5 * along * along - 1.5 * INFLOW * INFLOW))
    return jnp.array(values, jnp.float32)


def framed(center, top_row, bottom_row, left_col, right_col):
    middle = jnp.concatenate([left_col[..., :, None], center, right_col[..., :, None]], axis=-1)
    corner = jnp.zeros(top_row.shape[:-1] + (1,), top_row.dtype)
    upper = jnp.concatenate([corner, top_row, corner], axis=-1)[..., None, :]
    lower = jnp.concatenate([corner, bottom_row, corner], axis=-1)[..., None, :]
    return jnp.concatenate([upper, middle, lower], axis=-2)


def bordered(center, left_col, right_col):
    return jnp.concatenate([left_col[..., None], center, right_col[..., None]], axis=-1)


def assemble(eq_ext, neq_ext, recv_scale, inflow_side, outflow_side):
    size_x, size_y, size_z = recv_scale.shape
    factor = recv_scale[:, :, :, None, None, None]

    def neighbour(shift_x, shift_y, shift_z, face_id):
        window = (slice(1 + shift_x, 1 + shift_x + size_x), slice(1 + shift_y, 1 + shift_y + size_y), slice(1 + shift_z, 1 + shift_z + size_z), face_id)
        return eq_ext[window] + factor * neq_ext[window]

    plane_west = framed(neighbour(-1, 0, 0, 1), neighbour(-1, -1, 0, 1)[..., -1, :], neighbour(-1, 1, 0, 1)[..., 0, :], neighbour(-1, 0, -1, 1)[..., :, -1], neighbour(-1, 0, 1, 1)[..., :, 0])
    plane_east = framed(neighbour(1, 0, 0, 0), neighbour(1, -1, 0, 0)[..., -1, :], neighbour(1, 1, 0, 0)[..., 0, :], neighbour(1, 0, -1, 0)[..., :, -1], neighbour(1, 0, 1, 0)[..., :, 0])
    plane_south = bordered(neighbour(0, -1, 0, 3), neighbour(0, -1, -1, 3)[..., :, -1], neighbour(0, -1, 1, 3)[..., :, 0])
    plane_north = bordered(neighbour(0, 1, 0, 2), neighbour(0, 1, -1, 2)[..., :, -1], neighbour(0, 1, 1, 2)[..., :, 0])
    plane_below = neighbour(0, 0, -1, 5)
    plane_above = neighbour(0, 0, 1, 4)
    plane_west = jnp.where(inflow_side[:, None, None, None, None, None], inflow_column(FACE_SPEEDS[1])[:, None, None], plane_west)
    plane_east = jnp.where(outflow_side[:, None, None, None, None, None], inflow_column(FACE_SPEEDS[0])[:, None, None], plane_east)
    return plane_west, plane_east, plane_south, plane_north, plane_below, plane_above


def propagate(relaxed, planes):
    patch_total = relaxed.shape[0]
    extent = relaxed.shape[-1]
    padded = jnp.zeros((patch_total, 19, extent + 2, extent + 2, extent + 2), relaxed.dtype)
    padded = padded.at[:, :, 1:extent + 1, 1:extent + 1, 1:extent + 1].set(relaxed)
    plane_west, plane_east, plane_south, plane_north, plane_below, plane_above = planes
    for column, speed in enumerate(FACE_SPEEDS[1]):
        padded = padded.at[:, speed, 0, :, :].set(plane_west[:, column])
    for column, speed in enumerate(FACE_SPEEDS[0]):
        padded = padded.at[:, speed, extent + 1, :, :].set(plane_east[:, column])
    for column, speed in enumerate(FACE_SPEEDS[3]):
        padded = padded.at[:, speed, 1:extent + 1, 0, :].set(plane_south[:, column])
    for column, speed in enumerate(FACE_SPEEDS[2]):
        padded = padded.at[:, speed, 1:extent + 1, extent + 1, :].set(plane_north[:, column])
    for column, speed in enumerate(FACE_SPEEDS[5]):
        padded = padded.at[:, speed, 1:extent + 1, 1:extent + 1, 0].set(plane_below[:, column])
    for column, speed in enumerate(FACE_SPEEDS[4]):
        padded = padded.at[:, speed, 1:extent + 1, 1:extent + 1, extent + 1].set(plane_above[:, column])
    shifted = []
    for speed in range(19):
        step_x, step_y, step_z = VELOCITIES[speed]
        shifted.append(padded[:, speed, 1 - step_x:1 - step_x + extent, 1 - step_y:1 - step_y + extent, 1 - step_z:1 - step_z + extent])
    return jnp.stack(shifted, axis=1)


def lattice_order(values):
    trailing = values.shape[1:]
    lattice = values.reshape((N_BLOCKS, N_CROSS, FLOW_PATCHES, SPAN_PATCHES, DEPTH_PATCHES) + trailing)
    lattice = jnp.moveaxis(lattice, 2, 1)
    return lattice.reshape((N_BLOCKS * FLOW_PATCHES, N_CROSS * SPAN_PATCHES, DEPTH_PATCHES) + trailing)


def id_order(lattice):
    trailing = lattice.shape[3:]
    grouped = lattice.reshape((N_BLOCKS, FLOW_PATCHES, N_CROSS, SPAN_PATCHES, DEPTH_PATCHES) + trailing)
    grouped = jnp.moveaxis(grouped, 1, 2)
    return grouped.reshape((PATCHES,) + trailing)


def wrap_axis(values, axis_id):
    length = values.shape[axis_id]
    return jnp.concatenate([lax.slice_in_dim(values, length - 1, length, axis=axis_id), values, lax.slice_in_dim(values, 0, 1, axis=axis_id)], axis=axis_id)


def grouped(values):
    return values.reshape((N_BLOCKS * N_CROSS, PATCH_DEV) + values.shape[1:])


def reference(f_home, levels, plan):
    populations = f_home.reshape(PATCHES, 19, EDGE, EDGE, EDGE)
    fine_mask = levels == 1
    relax_rate = jnp.where(fine_mask, 1.0 / TAU_FINE, 1.0 / TAU_COARSE).astype(jnp.float32)
    send_scale = jnp.where(fine_mask, 1.0 / RESCALE, 1.0).astype(jnp.float32)
    recv_scale = lattice_order(jnp.where(fine_mask, RESCALE, 1.0).astype(jnp.float32))
    span_x = FLOW_PATCHES * N_BLOCKS
    position = jnp.arange(span_x, dtype=jnp.int32)

    def group_faces(pieces):
        relaxed, balance, density, velocity = collide(pieces[0], pieces[1])
        return face_payload(relaxed, balance, pieces[2])

    def group_step(pieces):
        fine_rate = jnp.full((PATCH_DEV,), 1.0 / TAU_FINE, jnp.float32)
        planes = pieces[3:]
        relaxed = collide(pieces[0], pieces[1])[0]
        moved = propagate(relaxed, planes)
        updated = propagate(collide(moved, fine_rate)[0], planes)
        return jnp.where(pieces[2][:, None, None, None, None], updated, moved)

    for round_id in range(STEPS):
        eq_faces, neq_faces = lax.map(group_faces, (grouped(populations), grouped(relax_rate), grouped(send_scale)))
        eq_ext = lattice_order(eq_faces.reshape((PATCHES,) + eq_faces.shape[2:]))
        neq_ext = lattice_order(neq_faces.reshape((PATCHES,) + neq_faces.shape[2:]))
        for axis_id in range(3):
            eq_ext = wrap_axis(eq_ext, axis_id)
            neq_ext = wrap_axis(neq_ext, axis_id)
        planes = assemble(eq_ext, neq_ext, recv_scale, position == 0, position == span_x - 1)
        planes = tuple(grouped(id_order(plane)) for plane in planes)
        populations = lax.map(group_step, (grouped(populations), grouped(relax_rate), grouped(fine_mask)) + planes)
        populations = populations.reshape(PATCHES, 19, EDGE, EDGE, EDGE)
    flattened = populations.reshape(PATCHES, 19, CELLS)
    return jnp.zeros_like(flattened).at[plan].set(flattened)
```

```python
import jax
import jax.numpy as jnp
from jax import lax
from jax.experimental import pallas as pl
from jax.experimental.pallas import tpu as pltpu
from jax.sharding import PartitionSpec as P

STEPS = 2
MESH = pl.DeviceIdType.MESH
VELOCITIES = (
    (0, 0, 0),
    (1, 0, 0),
    (-1, 0, 0),
    (0, 1, 0),
    (0, -1, 0),
    (0, 0, 1),
    (0, 0, -1),
    (1, 1, 0),
    (-1, -1, 0),
    (1, -1, 0),
    (-1, 1, 0),
    (1, 0, 1),
    (-1, 0, -1),
    (1, 0, -1),
    (-1, 0, 1),
    (0, 1, 1),
    (0, -1, -1),
    (0, 1, -1),
    (0, -1, 1),
)
WEIGHTS = (1.0 / 3.0,) + (1.0 / 18.0,) * 6 + (1.0 / 36.0,) * 12
PAIRS = tuple((q, q + 1) for q in range(1, 19, 2))
X_SPEEDS = ((1, 7, 9, 11, 13), (2, 8, 10, 12, 14))
Y_SPEEDS = ((3, 7, 10, 15, 17), (4, 8, 9, 16, 18))
TAU_COARSE = 0.55
TAU_FINE = 2.0 * TAU_COARSE - 0.5
RESCALE = TAU_FINE / (2.0 * TAU_COARSE)
INFLOW = 0.08
ROWS = 76


def inflow_value(speed):
    along = VELOCITIES[speed][0] * INFLOW
    return WEIGHTS[speed] * (1.0 + 3.0 * along + 4.5 * along * along - 1.5 * INFLOW * INFLOW)


def equilibrium(field):
    density = field[0]
    for q in range(1, 19):
        density = density + field[q]
    inverse = 1.0 / density
    velocity = []
    for axis in range(3):
        total = None
        for q in range(1, 19):
            sign = VELOCITIES[q][axis]
            if sign:
                if total is None:
                    total = field[q] if sign > 0 else -field[q]
                else:
                    total = total + field[q] if sign > 0 else total - field[q]
        velocity.append(total * inverse)
    ux, uy, uz = velocity
    base = 1.0 - 1.5 * (ux * ux + uy * uy + uz * uz)
    out = [None] * 19
    out[0] = WEIGHTS[0] * density * base
    for plus, minus in PAIRS:
        along = None
        for axis in range(3):
            sign = VELOCITIES[plus][axis]
            if sign:
                term = velocity[axis]
                if along is None:
                    along = term
                else:
                    along = along + term if sign > 0 else along - term
        even = base + 4.5 * along * along
        odd = 3.0 * along
        scale = WEIGHTS[plus] * density
        out[plus] = scale * (even + odd)
        out[minus] = scale * (even - odd)
    return out


def lattice_masks(shape):
    lane = lax.broadcasted_iota(jnp.int32, shape, len(shape) - 1)
    return lane, (lane // 8) % 8, lane % 8


def wide_roll(values, shift, axis):
    shift = shift % values.shape[axis]
    return values if shift == 0 else pltpu.roll(values, shift, axis)


def shifted(main, before, after, q):
    ex, ey, ez = VELOCITIES[q]
    lane, j, k = lattice_masks((1, 8, 128))
    if ex > 0:
        other = jnp.concatenate([before[None], main[:3]], axis=0)
        main = jnp.where(lane[None] < 64, main, other)
    elif ex < 0:
        other = jnp.concatenate([main[1:], after[None]], axis=0)
        main = jnp.where(lane[None] >= 64, main, other)
    turn = 64 if ex else 0
    here = main[:, 1:5].reshape(16, 8, 128)
    if ey > 0:
        there = main[:, 0:4].reshape(16, 8, 128)
        here = jnp.where(j > 0, wide_roll(here, turn + 8, 2), wide_roll(there, turn - 56, 2))
        turn = 0
    elif ey < 0:
        there = main[:, 2:6].reshape(16, 8, 128)
        here = jnp.where(j < 7, wide_roll(here, turn - 8, 2), wide_roll(there, turn + 56, 2))
        turn = 0
    if ez > 0:
        over = wide_roll(wide_roll(here, 1, 1), turn - 7, 2)
        here = jnp.where(k > 0, wide_roll(here, turn + 1, 2), over)
    elif ez < 0:
        over = wide_roll(wide_roll(here, 7, 1), turn + 7, 2)
        here = jnp.where(k < 7, wide_roll(here, turn - 1, 2), over)
    else:
        here = wide_roll(here, turn, 2)
    return here


def shifted_inside(main, q):
    ex, ey, ez = VELOCITIES[q]
    shape = (4, 1, 8, 128)
    lane, j, k = lattice_masks(shape)
    high = lax.broadcasted_iota(jnp.int32, shape, 0)
    inside = lane >= 0
    if ex > 0:
        other = jnp.concatenate([main[:1], main[:3]], axis=0)
        main = jnp.where(lane < 64, main, other)
        inside = inside & (high * 128 + lane >= 64)
    elif ex < 0:
        other = jnp.concatenate([main[1:], main[3:]], axis=0)
        main = jnp.where(lane >= 64, main, other)
        inside = inside & (high * 128 + lane < 448)
    if ey:
        inside = inside & ((j > 0) if ey > 0 else (j < 7))
    if ez:
        inside = inside & ((k > 0) if ez > 0 else (k < 7))
    turn = (64 if ex else 0) + 8 * ey + ez
    moved = wide_roll(main.reshape(16, 8, 128), turn, 2)
    return moved.reshape(4, 4, 8, 128), inside


def lbm_kernel(blocks, f_hbm, levels, x_out, raw, state, both, work, pack_x, halo_x, coef, load_sem, send_sem, recv_sem):
    b = lax.axis_index("blocks")
    c = lax.axis_index("cross")
    has_low, has_high = b > 0, b < blocks - 1
    low, high = jnp.maximum(b - 1, 0), jnp.minimum(b + 1, blocks - 1)

    for ih in range(4):
        pltpu.make_async_copy(
            f_hbm.at[:, :, pl.ds(128 * ih, 128)], raw.at[ih, :, pl.ds(0, 19)], load_sem.at[ih]
        ).start()

    barrier = pltpu.get_barrier_semaphore()

    def greet(device):
        pl.semaphore_signal(barrier, inc=1, device_id=device, device_id_type=MESH)

    greet((b, 1 - c))

    @pl.when(has_low)
    def _():
        greet((low, c))
        greet((low, 1 - c))

    @pl.when(has_high)
    def _():
        greet((high, c))
        greet((high, 1 - c))

    sublane = lax.broadcasted_iota(jnp.int32, (8, 128), 0)
    for py in range(4):
        fine = jnp.zeros((8, 128), jnp.float32)
        for pz in range(8):
            fine = jnp.where(sublane == pz, levels[py * 8 + pz].astype(jnp.float32), fine)
        is_fine = fine > 0.5
        coef[0, py] = fine
        coef[1, py] = jnp.where(is_fine, (1.0 - 1.0 / TAU_FINE) / RESCALE, 1.0 - 1.0 / TAU_COARSE)
        coef[2, py] = jnp.where(is_fine, 1.0 - 1.0 / TAU_FINE, RESCALE * (1.0 - 1.0 / TAU_COARSE))

    for step in range(STEPS):
        for side in range(2):

            @pl.when(jnp.logical_not(has_low if side == 0 else has_high))
            def _():
                for n, q in enumerate(X_SPEEDS[side]):
                    halo_x[step, side, n] = jnp.full((6, 8, 128), inflow_value(q), jnp.float32)

    for ih in range(4):
        pltpu.make_async_copy(
            f_hbm.at[:, :, pl.ds(128 * ih, 128)], raw.at[ih, :, pl.ds(0, 19)], load_sem.at[ih]
        ).wait()
    pl.semaphore_wait(
        barrier, 1 + 2 * has_low.astype(jnp.int32) + 2 * has_high.astype(jnp.int32)
    )

    lane = lax.broadcasted_iota(jnp.int32, (4, 8, 128), 2)
    pending = []
    for step in range(STEPS):

        def relax_both(pos, carry):
            ih, py = pos // 4, pos % 4
            rows = pl.ds(pl.multiple_of(py * 8, 8), 8)
            if step:
                field = [state[q, ih, rows, :] for q in range(19)]
            else:
                flat = raw.at[ih].reshape(768, 128)
                field = [flat[pl.ds(py * 192 + q, 8, stride=24), :] for q in range(19)]
            balance = equilibrium(field)
            for_coarse, for_fine = coef[1, py], coef[2, py]
            for q in range(19):
                away = field[q] - balance[q]
                both[step, 0, q, ih, py + 1] = balance[q] + for_coarse * away
                both[step, 1, q, ih, py + 1] = balance[q] + for_fine * away
            return carry

        lax.fori_loop(0, 16, relax_both, 0)

        copies = []

        def add(src, dst, device, send_if, recv_if):
            index = len(copies)
            copy = pltpu.make_async_remote_copy(
                src_ref=src,
                dst_ref=dst,
                send_sem=send_sem.at[step, index],
                recv_sem=recv_sem.at[step, index],
                device_id=device,
                device_id_type=MESH,
            )
            copies.append((send_if, recv_if, copy))

        for side in range(2):
            edge = 3 if side == 0 else 0
            for n, q in enumerate(X_SPEEDS[side]):
                first = both[step, 0, q, edge, 1:5]
                second = pltpu.roll(both[step, 1, q, edge, 1:5], 64, 2)
                keep = lane >= 64 if side == 0 else lane < 64
                pack_x[step, side, n] = jnp.where(keep, first, second)
        for side in range(2):
            target = high if side == 0 else low
            send_if, recv_if = (has_high, has_low) if side == 0 else (has_low, has_high)
            add(
                pack_x.at[step, side],
                halo_x.at[step, side, :, pl.ds(1, 4)],
                (target, c),
                send_if,
                recv_if,
            )
            for n, q in enumerate(X_SPEEDS[side]):
                ey = VELOCITIES[q][1]
                if ey:
                    py, slot = (3, 0) if ey > 0 else (0, 5)
                    add(
                        pack_x.at[step, side, n, py],
                        halo_x.at[step, side, n, slot],
                        (target, 1 - c),
                        send_if,
                        recv_if,
                    )
        for side in range(2):
            py, slot = (4, 0) if side == 0 else (1, 5)
            for q in Y_SPEEDS[side]:
                add(
                    both.at[step, :, q, :, py],
                    both.at[step, :, q, :, slot],
                    (b, 1 - c),
                    None,
                    None,
                )
        for send_if, recv_if, copy in copies:
            if send_if is None:
                copy.start()
            else:
                pl.when(send_if)(copy.start)
        for send_if, recv_if, copy in copies:
            if recv_if is None:
                copy.wait_recv()
            else:
                pl.when(recv_if)(copy.wait_recv)
        pending += copies

        fine = coef[0] > 0.5
        for q in range(19):
            ex = VELOCITIES[q][0]
            result = []
            for kind in range(2):
                before = after = None
                if ex > 0:
                    before = halo_x[step, 0, X_SPEEDS[0].index(q)]
                    before = pltpu.roll(before, 64, 2) if kind else before
                elif ex < 0:
                    after = halo_x[step, 1, X_SPEEDS[1].index(q)]
                    after = pltpu.roll(after, 64, 2) if kind else after
                main = both[step, kind, q]
                result.append(shifted(main, before, after, q).reshape(4, 4, 8, 128))
            state[q] = jnp.where(fine[None], result[1], result[0]).reshape(4, 32, 128)

        def relax_again(pos, carry):
            ih, py = pos // 4, pos % 4
            rows = pl.ds(pl.multiple_of(py * 8, 8), 8)
            field = [state[q, ih, rows, :] for q in range(19)]
            balance = equilibrium(field)
            for q in range(19):
                work[q, ih, py] = field[q] + (1.0 / TAU_FINE) * (balance[q] - field[q])
            return carry

        lax.fori_loop(0, 16, relax_again, 0)
        for q in range(19):
            moved, inside = shifted_inside(work[q], q)
            kept = state[q].reshape(4, 4, 8, 128)
            result = jnp.where(inside & fine[None], moved, kept).reshape(4, 32, 128)
            if step == STEPS - 1:
                x_out[pl.ds(4 * q, 4)] = result
            else:
                state[q] = result

    for send_if, recv_if, copy in pending:
        if send_if is None:
            copy.wait_send()
        else:
            pl.when(send_if)(copy.wait_send)


def row_holder(row):
    spare = row - 64
    x, e = spare // 3, spare % 3
    chip = 16 * x + 4 * ((e + x) % 4) + (e + 3 * x) % 4
    return jnp.where(row < 64, row, chip), jnp.where(row < 64, 1, 0)


def row_of(b, c):
    x, z, y = b // 16, (b // 4) % 4, b % 4
    e = (z + 4 - x) % 4
    spare = (e < 3) & (y == (e + 3 * x) % 4)
    row = jnp.where(c == 1, b, 64 + 3 * x + e)
    return row, (c == 1) | spare


def migrate_kernel(
    devices, x_ref, plan_ref, out_ref, plan_all, plan_turned, inv_vec, inv_smem, gathered, ordered,
    local_sem, plan_send, plan_recv, spread_send, spread_recv, home_send, home_recv,
):
    b = lax.axis_index("blocks")
    c = lax.axis_index("cross")
    me = 2 * b + c
    my_row, is_mid = row_of(b, c)
    barrier = pltpu.get_barrier_semaphore()

    def each_other(body):
        def step(k, carry):
            other = (me + k) % devices
            body(other, (other // 2, other % 2))
            return carry

        lax.fori_loop(1, devices, step, 0)

    each_other(
        lambda other, device: pl.semaphore_signal(
            barrier, inc=1, device_id=device, device_id_type=MESH
        )
    )
    plan_all[me] = plan_ref[...]
    pl.semaphore_wait(barrier, devices - 1)

    def send_plan(other, device):
        pltpu.make_async_remote_copy(
            src_ref=plan_ref,
            dst_ref=plan_all.at[me],
            send_sem=plan_send,
            recv_sem=plan_recv,
            device_id=device,
            device_id_type=MESH,
        ).start()

    each_other(send_plan)

    def send_row(k, carry):
        row = (my_row + 1 + k) % ROWS
        device = row_holder(row)

        @pl.when((device[0] != b) | (device[1] != c))
        def _():
            pltpu.make_async_remote_copy(
                src_ref=x_ref.at[row],
                dst_ref=gathered.at[pl.ds(pl.multiple_of(me * 32, 32), 32)],
                send_sem=spread_send,
                recv_sem=spread_recv,
                device_id=device,
                device_id_type=MESH,
            ).start()

        return carry

    lax.fori_loop(0, ROWS, send_row, 0)

    def wait_for(sem, blocks_of_rows):
        part = gathered.at[pl.ds(0, 32 * blocks_of_rows)]
        pltpu.make_async_copy(part, part, sem).wait()

    others = plan_all.at[pl.ds(0, devices - 1)]
    pltpu.make_async_copy(others, others, plan_recv).wait()

    @pl.when(is_mid)
    def _():
        gathered[pl.ds(pl.multiple_of(me * 32, 32), 32), :] = x_ref[my_row]
        plans = plan_all[:, 0, :]
        plan_turned[...] = plans.T
        sub = lax.broadcasted_iota(jnp.int32, (128, 128), 0)
        lane = lax.broadcasted_iota(jnp.int32, (128, 128), 1)

        def place(p, carry):
            plans, total = carry
            owner = plan_turned[pl.ds(p, 1), :] // 32
            hot = jnp.where(owner == sub, 1.0, 0.0)
            slot = plans[:, 0:1] % 32
            value = jnp.where(slot == lane, sub, jnp.where(slot + 32 == lane, p, 0))
            total = total + jnp.dot(
                hot.astype(jnp.bfloat16),
                value.astype(jnp.float32).astype(jnp.bfloat16),
                preferred_element_type=jnp.float32,
            )
            return pltpu.roll(plans, 127, 1), total

        _, total = lax.fori_loop(0, 32, place, (plans, jnp.zeros((128, 128), jnp.float32)))
        total = total.astype(jnp.int32)
        inv_vec[...] = jnp.clip(total * 32 + pltpu.roll(total, 96, 1), 0, 32 * devices - 1)
        move = pltpu.make_async_copy(inv_vec, inv_smem, local_sem)
        move.start()
        move.wait()
        wait_for(spread_recv, devices - 1)

        def place_at(owner):
            return ordered.at[pl.ds(pl.multiple_of(owner * 32, 32), 32)]

        def target():
            return out_ref.at[my_row]

        def send_owner(owner):
            pltpu.make_async_remote_copy(
                src_ref=place_at(owner),
                dst_ref=target(),
                send_sem=home_send,
                recv_sem=home_recv,
                device_id=(owner // 2, owner % 2),
                device_id_type=MESH,
            ).start()

        def pick(k, carry):
            owner = (me + k) % devices
            for u in range(32):
                index = inv_smem[owner, u]
                ordered[pl.ds(owner * 32 + u, 1), :] = gathered[pl.ds(index, 1), :]

            @pl.when(k > 1)
            def _():
                send_owner((me + k - 1) % devices)

            return carry

        lax.fori_loop(1, devices + 1, pick, 0)
        out_ref[my_row] = ordered[pl.ds(pl.multiple_of(me * 32, 32), 32), :]
        wait_for(home_send, devices - 1)
        wait_for(spread_send, ROWS - 1)
        wait_for(home_recv, ROWS - 1)

    @pl.when(jnp.logical_not(is_mid))
    def _():
        wait_for(spread_send, ROWS)
        wait_for(home_recv, ROWS)

    pltpu.make_async_copy(others, others, plan_send).wait()


def lbm_call(f_home, levels):
    blocks = lax.axis_size("blocks")
    vmem = pl.BlockSpec(memory_space=pltpu.VMEM)
    return pl.pallas_call(
        lambda *refs: lbm_kernel(blocks, *refs),
        out_shape=jax.ShapeDtypeStruct((ROWS, 32, 128), jnp.float32),
        in_specs=[pl.BlockSpec(memory_space=pl.ANY), pl.BlockSpec(memory_space=pltpu.SMEM)],
        out_specs=vmem,
        scratch_shapes=[
            pltpu.VMEM((4, 32, 24, 128), jnp.float32),
            pltpu.VMEM((19, 4, 32, 128), jnp.float32),
            pltpu.VMEM((STEPS, 2, 19, 4, 6, 8, 128), jnp.float32),
            pltpu.VMEM((19, 4, 4, 8, 128), jnp.float32),
            pltpu.VMEM((STEPS, 2, 5, 4, 8, 128), jnp.float32),
            pltpu.VMEM((STEPS, 2, 5, 6, 8, 128), jnp.float32),
            pltpu.VMEM((3, 4, 8, 128), jnp.float32),
            pltpu.SemaphoreType.DMA((4,)),
            pltpu.SemaphoreType.DMA((STEPS, 16)),
            pltpu.SemaphoreType.DMA((STEPS, 16)),
        ],
        compiler_params=pltpu.CompilerParams(
            collective_id=0, has_side_effects=True, vmem_limit_bytes=60 * 1024 * 1024
        ),
        name="lbm",
    )(f_home, levels)


def body(f_home, levels, plan):
    blocks = lax.axis_size("blocks")
    devices = 2 * blocks
    vmem = pl.BlockSpec(memory_space=pltpu.VMEM)
    state = lbm_call(f_home, levels)
    rows = pl.pallas_call(
        lambda *refs: migrate_kernel(devices, *refs),
        out_shape=jax.ShapeDtypeStruct((ROWS, 32, 128), jnp.float32),
        in_specs=[vmem, vmem],
        out_specs=vmem,
        scratch_shapes=[
            pltpu.VMEM((devices, 1, 128), jnp.int32),
            pltpu.VMEM((128, 128), jnp.int32),
            pltpu.VMEM((128, 128), jnp.int32),
            pltpu.SMEM((128, 128), jnp.int32),
            pltpu.VMEM((devices * 32, 128), jnp.float32),
            pltpu.VMEM((devices * 32, 128), jnp.float32),
        ]
        + [pltpu.SemaphoreType.DMA] * 7,
        compiler_params=pltpu.CompilerParams(
            collective_id=1, has_side_effects=True, vmem_limit_bytes=60 * 1024 * 1024
        ),
        name="migrate",
    )(state, jnp.pad(plan, (0, 96)).reshape(1, 128))
    return rows.reshape(19, 4, 32, 128).transpose(2, 0, 1, 3).reshape(32, 19, 512)


def solution(mesh):
    spec = P(("blocks", "cross"))
    return jax.shard_map(
        body, mesh=mesh, in_specs=(spec, spec, spec), out_specs=spec, check_vma=False
    )
```

```python
import jax
import jax.numpy as jnp
from jax import lax
from jax.experimental import pallas as pl
from jax.experimental.pallas import tpu as pltpu
from jax.sharding import PartitionSpec as P

STEPS = 2
MESH = pl.DeviceIdType.MESH
VELOCITIES = (
    (0, 0, 0),
    (1, 0, 0),
    (-1, 0, 0),
    (0, 1, 0),
    (0, -1, 0),
    (0, 0, 1),
    (0, 0, -1),
    (1, 1, 0),
    (-1, -1, 0),
    (1, -1, 0),
    (-1, 1, 0),
    (1, 0, 1),
    (-1, 0, -1),
    (1, 0, -1),
    (-1, 0, 1),
    (0, 1, 1),
    (0, -1, -1),
    (0, 1, -1),
    (0, -1, 1),
)
WEIGHTS = (1.0 / 3.0,) + (1.0 / 18.0,) * 6 + (1.0 / 36.0,) * 12
PAIRS = tuple((q, q + 1) for q in range(1, 19, 2))
X_SPEEDS = ((1, 7, 9, 11, 13), (2, 8, 10, 12, 14))
Y_SPEEDS = ((3, 7, 10, 15, 17), (4, 8, 9, 16, 18))
TAU_COARSE = 0.55
TAU_FINE = 2.0 * TAU_COARSE - 0.5
RESCALE = TAU_FINE / (2.0 * TAU_COARSE)
INFLOW = 0.08
ROWS = 76
UNITS = 48
VMEM_LIMIT = 28 * 1024 * 1024


def inflow_value(speed):
    along = VELOCITIES[speed][0] * INFLOW
    return WEIGHTS[speed] * (1.0 + 3.0 * along + 4.5 * along * along - 1.5 * INFLOW * INFLOW)


def equilibrium(field):
    density = field[0]
    for q in range(1, 19):
        density = density + field[q]
    inverse = 1.0 / density
    velocity = []
    for axis in range(3):
        total = None
        for q in range(1, 19):
            sign = VELOCITIES[q][axis]
            if sign:
                if total is None:
                    total = field[q] if sign > 0 else -field[q]
                else:
                    total = total + field[q] if sign > 0 else total - field[q]
        velocity.append(total * inverse)
    ux, uy, uz = velocity
    base = 1.0 - 1.5 * (ux * ux + uy * uy + uz * uz)
    out = [None] * 19
    out[0] = WEIGHTS[0] * density * base
    for plus, minus in PAIRS:
        along = None
        for axis in range(3):
            sign = VELOCITIES[plus][axis]
            if sign:
                term = velocity[axis]
                if along is None:
                    along = term
                else:
                    along = along + term if sign > 0 else along - term
        even = base + 4.5 * along * along
        odd = 3.0 * along
        scale = WEIGHTS[plus] * density
        out[plus] = scale * (even + odd)
        out[minus] = scale * (even - odd)
    return out


def lattice_masks(shape):
    lane = lax.broadcasted_iota(jnp.int32, shape, len(shape) - 1)
    return lane, (lane // 8) % 8, lane % 8


def wide_roll(values, shift, axis):
    shift = shift % values.shape[axis]
    return values if shift == 0 else pltpu.roll(values, shift, axis)


def shifted(main, before, after, q):
    ex, ey, ez = VELOCITIES[q]
    lane, j, k = lattice_masks((1, 8, 128))
    if ex > 0:
        other = jnp.concatenate([before[None], main[:3]], axis=0)
        main = jnp.where(lane[None] < 64, main, other)
    elif ex < 0:
        other = jnp.concatenate([main[1:], after[None]], axis=0)
        main = jnp.where(lane[None] >= 64, main, other)
    turn = 64 if ex else 0
    here = main[:, 1:5].reshape(16, 8, 128)
    if ey > 0:
        there = main[:, 0:4].reshape(16, 8, 128)
        here = jnp.where(j > 0, wide_roll(here, turn + 8, 2), wide_roll(there, turn - 56, 2))
        turn = 0
    elif ey < 0:
        there = main[:, 2:6].reshape(16, 8, 128)
        here = jnp.where(j < 7, wide_roll(here, turn - 8, 2), wide_roll(there, turn + 56, 2))
        turn = 0
    if ez > 0:
        over = wide_roll(wide_roll(here, 1, 1), turn - 7, 2)
        here = jnp.where(k > 0, wide_roll(here, turn + 1, 2), over)
    elif ez < 0:
        over = wide_roll(wide_roll(here, 7, 1), turn + 7, 2)
        here = jnp.where(k < 7, wide_roll(here, turn - 1, 2), over)
    else:
        here = wide_roll(here, turn, 2)
    return here


def shifted_inside(main, q):
    ex, ey, ez = VELOCITIES[q]
    shape = (4, 1, 8, 128)
    lane, j, k = lattice_masks(shape)
    high = lax.broadcasted_iota(jnp.int32, shape, 0)
    inside = lane >= 0
    if ex > 0:
        other = jnp.concatenate([main[:1], main[:3]], axis=0)
        main = jnp.where(lane < 64, main, other)
        inside = inside & (high * 128 + lane >= 64)
    elif ex < 0:
        other = jnp.concatenate([main[1:], main[3:]], axis=0)
        main = jnp.where(lane >= 64, main, other)
        inside = inside & (high * 128 + lane < 448)
    if ey:
        inside = inside & ((j > 0) if ey > 0 else (j < 7))
    if ez:
        inside = inside & ((k > 0) if ez > 0 else (k < 7))
    turn = (64 if ex else 0) + 8 * ey + ez
    moved = wide_roll(main.reshape(16, 8, 128), turn, 2)
    return moved.reshape(4, 4, 8, 128), inside


def lbm_steps(
    blocks, f_hbm, levels_hbm, plan_hbm, rows, plan_all, levels, plan, raw, state, both, work, pack_x, halo_x, coef,
    load_sem, send_sem, recv_sem, round_send, round_recv,
):
    b = lax.axis_index("blocks")
    c = lax.axis_index("cross")
    has_low, has_high = b > 0, b < blocks - 1
    low, high = jnp.maximum(b - 1, 0), jnp.minimum(b + 1, blocks - 1)

    loads = [
        pltpu.make_async_copy(
            f_hbm.at[:, :, pl.ds(128 * ih, 128)], raw.at[ih], load_sem.at[ih]
        )
        for ih in range(4)
    ]
    numbers = [
        pltpu.make_async_copy(levels_hbm, levels, load_sem.at[4]),
        pltpu.make_async_copy(plan_hbm, plan, load_sem.at[5]),
    ]
    for load in numbers + loads:
        load.start()

    barrier = pltpu.get_barrier_semaphore()

    def greet(device):
        pl.semaphore_signal(barrier, inc=1, device_id=device, device_id_type=MESH)

    greet((b, 1 - c))

    @pl.when(has_low)
    def _():
        greet((low, c))
        greet((low, 1 - c))

    @pl.when(has_high)
    def _():
        greet((high, c))
        greet((high, 1 - c))

    for load in numbers:
        load.wait()
    sublane = lax.broadcasted_iota(jnp.int32, (8, 128), 0)
    for py in range(4):
        fine = jnp.zeros((8, 128), jnp.float32)
        for pz in range(8):
            fine = jnp.where(sublane == pz, levels[py * 8 + pz].astype(jnp.float32), fine)
        is_fine = fine > 0.5
        coef[0, py] = fine
        coef[1, py] = jnp.where(is_fine, (1.0 - 1.0 / TAU_FINE) / RESCALE, 1.0 - 1.0 / TAU_COARSE)
        coef[2, py] = jnp.where(is_fine, 1.0 - 1.0 / TAU_FINE, RESCALE * (1.0 - 1.0 / TAU_COARSE))

    for step in range(STEPS):
        for side in range(2):

            @pl.when(jnp.logical_not(has_low if side == 0 else has_high))
            def _():
                for n, q in enumerate(X_SPEEDS[side]):
                    halo_x[step, side, n] = jnp.full((6, 8, 128), inflow_value(q), jnp.float32)

    plan_row = jnp.zeros((1, 128), jnp.int32)
    plan_lane = lax.broadcasted_iota(jnp.int32, (1, 128), 1)
    for p in range(32):
        plan_row = jnp.where(plan_lane == p, plan[p], plan_row)
    plan_all[64 * c + b] = plan_row

    def line(axis):
        stride = (16, 4, 1)[axis]
        at = (b // stride) % 4
        return [b + stride * ((at + k) % 4 - at) for k in (1, 2, 3)]

    for axis in range(3):
        for chip in line(axis):
            greet((chip, c))

    def plan_round(number):
        size = (1, 4, 16, 64)[number]
        part = plan_all.at[pl.ds(64 * c + (b // size) * size, size)]
        peers = [(b, 1 - c)] if number == 3 else [(chip, c) for chip in line(2 - number)]
        copies = [
            pltpu.make_async_remote_copy(
                src_ref=part,
                dst_ref=part,
                send_sem=round_send.at[number],
                recv_sem=round_recv.at[number],
                device_id=peer,
                device_id_type=MESH,
            )
            for peer in peers
        ]
        for copy in copies:
            copy.start()

    def end_round(number):
        moved = plan_all.at[pl.ds(0, (3, 12, 48, 64)[number])]
        pltpu.make_async_copy(moved, moved, round_recv.at[number]).wait()
        pltpu.make_async_copy(moved, moved, round_send.at[number]).wait()

    for load in loads:
        load.wait()
    pl.semaphore_wait(
        barrier, 10 + 2 * has_low.astype(jnp.int32) + 2 * has_high.astype(jnp.int32)
    )
    plan_round(0)

    lane = lax.broadcasted_iota(jnp.int32, (4, 8, 128), 2)
    pending = []
    for step in range(STEPS):

        def relax_both(pos, carry):
            ih, py = pos // 4, pos % 4
            rows_of_py = pl.ds(pl.multiple_of(py * 8, 8), 8)
            if step:
                field = [state[q, ih, rows_of_py, :] for q in range(19)]
            else:
                field = [raw[ih, q, rows_of_py, :] for q in range(19)]
            balance = equilibrium(field)
            for_coarse, for_fine = coef[1, py], coef[2, py]
            for q in range(19):
                away = field[q] - balance[q]
                both[step, 0, q, ih, py + 1] = balance[q] + for_coarse * away
                both[step, 1, q, ih, py + 1] = balance[q] + for_fine * away
            return carry

        lax.fori_loop(0, 16, relax_both, 0)

        copies = []

        def add(src, dst, device, send_if, recv_if):
            index = len(copies)
            copy = pltpu.make_async_remote_copy(
                src_ref=src,
                dst_ref=dst,
                send_sem=send_sem.at[step, index],
                recv_sem=recv_sem.at[step, index],
                device_id=device,
                device_id_type=MESH,
            )
            copies.append((send_if, recv_if, copy))

        for side in range(2):
            edge = 3 if side == 0 else 0
            for n, q in enumerate(X_SPEEDS[side]):
                first = both[step, 0, q, edge, 1:5]
                second = pltpu.roll(both[step, 1, q, edge, 1:5], 64, 2)
                keep = lane >= 64 if side == 0 else lane < 64
                pack_x[step, side, n] = jnp.where(keep, first, second)
        for side in range(2):
            target = high if side == 0 else low
            send_if, recv_if = (has_high, has_low) if side == 0 else (has_low, has_high)
            add(
                pack_x.at[step, side],
                halo_x.at[step, side, :, pl.ds(1, 4)],
                (target, c),
                send_if,
                recv_if,
            )
            for n, q in enumerate(X_SPEEDS[side]):
                ey = VELOCITIES[q][1]
                if ey:
                    py, slot = (3, 0) if ey > 0 else (0, 5)
                    add(
                        pack_x.at[step, side, n, py],
                        halo_x.at[step, side, n, slot],
                        (target, 1 - c),
                        send_if,
                        recv_if,
                    )
        for side in range(2):
            py, slot = (4, 0) if side == 0 else (1, 5)
            for q in Y_SPEEDS[side]:
                add(
                    both.at[step, :, q, :, py],
                    both.at[step, :, q, :, slot],
                    (b, 1 - c),
                    None,
                    None,
                )
        for send_if, recv_if, copy in copies:
            if send_if is None:
                copy.start()
            else:
                pl.when(send_if)(copy.start)
        if step == 0:
            end_round(0)
            plan_round(1)
        for send_if, recv_if, copy in copies:
            if recv_if is None:
                copy.wait_recv()
            else:
                pl.when(recv_if)(copy.wait_recv)
        pending += copies
        if step == 0:
            end_round(1)
            plan_round(2)
        else:
            end_round(3)

        fine = coef[0] > 0.5
        for q in range(19):
            ex = VELOCITIES[q][0]
            result = []
            for kind in range(2):
                before = after = None
                if ex > 0:
                    before = halo_x[step, 0, X_SPEEDS[0].index(q)]
                    before = pltpu.roll(before, 64, 2) if kind else before
                elif ex < 0:
                    after = halo_x[step, 1, X_SPEEDS[1].index(q)]
                    after = pltpu.roll(after, 64, 2) if kind else after
                main = both[step, kind, q]
                result.append(shifted(main, before, after, q).reshape(4, 4, 8, 128))
            state[q] = jnp.where(fine[None], result[1], result[0]).reshape(4, 32, 128)

        if step == 0:
            end_round(2)
            plan_round(3)

        def relax_again(pos, carry):
            ih, py = pos // 4, pos % 4
            rows_of_py = pl.ds(pl.multiple_of(py * 8, 8), 8)
            field = [state[q, ih, rows_of_py, :] for q in range(19)]
            balance = equilibrium(field)
            for q in range(19):
                work[q, ih, py] = field[q] + (1.0 / TAU_FINE) * (balance[q] - field[q])
            return carry

        lax.fori_loop(0, 16, relax_again, 0)
        for q in range(19):
            moved, inside = shifted_inside(work[q], q)
            kept = state[q].reshape(4, 4, 8, 128)
            result = jnp.where(inside & fine[None], moved, kept).reshape(4, 32, 128)
            if step == STEPS - 1:
                rows[pl.ds(4 * q, 4)] = result
            else:
                state[q] = result

    def drain():
        for send_if, recv_if, copy in pending:
            if send_if is None:
                copy.wait_send()
            else:
                pl.when(send_if)(copy.wait_send)

    return drain


def spare_unit(b):
    place = (b // 16 + (b // 4) % 4 + b % 4) % 4
    return jnp.minimum((b // 4) * 3 + place, UNITS - 1), place < 3


def chip_at(b, k):
    dx = k % 4
    dz = (dx + k // 4) % 4
    dy = (dz + k // 16) % 4
    return 16 * ((b // 16 + dx) % 4) + 4 * (((b // 4) % 4 + dz) % 4) + (b % 4 + dy) % 4


def quarters(parts, sign):
    quarter = lax.broadcasted_iota(jnp.int32, parts[0].shape, parts[0].ndim - 1) // 32
    out = []
    for h in range(4):
        total = parts[h]
        for m in range(4):
            if m != h:
                total = jnp.where(quarter == m, wide_roll(parts[m], 32 * (m - h), total.ndim - 1), total)
        out.append(total)
    return out


def migrate(
    chips, out_ref, rows, plan_all, plan_turned, inv_vec, inv_smem, gathered, ordered, unit_out, unit_in, unit_back,
    local_sem, row_send, unit_send, spread_recv, home_send, home_recv, unit_recv,
):
    b = lax.axis_index("blocks")
    c = lax.axis_index("cross")
    source = 64 * c + b
    my_unit, has_unit = spare_unit(b)
    is_spare = (c == 0) & has_unit
    is_main = c == 1

    def remote(src, dst, send, recv, device):
        pltpu.make_async_remote_copy(
            src_ref=src, dst_ref=dst, send_sem=send, recv_sem=recv, device_id=device, device_id_type=MESH
        ).start()

    def block(ref, index, size):
        return ref.at[pl.ds(pl.multiple_of(index * size, size), size)]

    spare_rows = rows[pl.ds(64, 12)].reshape(12, 4, 8, 128)
    for h, part in enumerate(quarters([spare_rows[:, m] for m in range(4)], 1)):
        unit_out[:, h] = part

    def spread(k, carry):
        chip = chip_at(b, k)

        @pl.when((k > 0) | (c == 0))
        def _():
            remote(rows.at[chip], block(gathered, source, 32), row_send, spread_recv, (chip, 1))

        unit, wanted = spare_unit(chip)

        @pl.when(wanted & ((k > 0) | (c == 1)))
        def _():
            remote(unit_out.at[unit // 4, unit % 4], block(unit_in, source, 8), unit_send, spread_recv, (chip, 0))

        return carry

    lax.fori_loop(0, chips, spread, 0)

    def wait_rows(sem, count):
        part = gathered.at[pl.ds(0, 32 * count)]
        pltpu.make_async_copy(part, part, sem).wait()

    def wait_units(sem, count):
        part = unit_in.at[pl.ds(0, 8 * count)]
        pltpu.make_async_copy(part, part, sem).wait()

    def find_slots():
        plans = plan_all[:, 0, :]
        plan_turned[...] = plans.T
        sub = lax.broadcasted_iota(jnp.int32, (128, 128), 0)
        lane = lax.broadcasted_iota(jnp.int32, (128, 128), 1)

        def place(p, carry):
            plans, total = carry
            owner = plan_turned[pl.ds(p, 1), :] // 32
            hot = jnp.where(owner == sub, 1.0, 0.0)
            slot = plans[:, 0:1] % 32
            value = jnp.where(slot == lane, sub, jnp.where(slot + 32 == lane, p, 0))
            total = total + jnp.dot(
                hot.astype(jnp.bfloat16),
                value.astype(jnp.float32).astype(jnp.bfloat16),
                preferred_element_type=jnp.float32,
            )
            return pltpu.roll(plans, 127, 1), total

        _, total = lax.fori_loop(0, 32, place, (plans, jnp.zeros((128, 128), jnp.float32)))
        total = total.astype(jnp.int32)
        inv_vec[...] = jnp.clip(total * 32 + pltpu.roll(total, 96, 1), 0, 64 * chips - 1)
        move = pltpu.make_async_copy(inv_vec, inv_smem, local_sem)
        move.start()
        move.wait()

    def pick(chip, core):
        owner = 2 * chip + core
        for u in range(32):
            index = inv_smem[owner, u]
            ordered[pl.ds(owner * 32 + u, 1), :] = gathered[pl.ds(index, 1), :]

    my_place = out_ref.at[b // 4, :, pl.ds(pl.multiple_of((b % 4) * 128, 128), 128)]

    @pl.when(is_main)
    def _():
        find_slots()
        gathered[pl.ds(pl.multiple_of(source * 32, 32), 32), :] = rows[b]
        wait_rows(spread_recv, 2 * chips - 1)

        def send(chip, core):
            remote(block(ordered, 2 * chip + core, 32), my_place, home_send, home_recv, (chip, core))

        def step(k, carry):
            chip = chip_at(b, k % chips)
            pick(chip, 0)
            pick(chip, 1)

            @pl.when(k > 1)
            def _():
                before = chip_at(b, k - 1)
                send(before, 0)
                send(before, 1)

            return carry

        lax.fori_loop(1, chips + 1, step, 0)
        out_ref[b // 4, :, pl.ds(pl.multiple_of((b % 4) * 128, 128), 128)] = ordered[
            pl.ds(pl.multiple_of((2 * b + 1) * 32, 32), 32), :
        ]
        send(b, 0)
        wait_rows(home_send, 2 * chips - 1)
        wait_rows(row_send, chips - 1)
        wait_units(unit_send, UNITS)
        wait_rows(home_recv, chips - 1)
        wait_units(unit_recv, UNITS)

    @pl.when(is_spare)
    def _():
        find_slots()
        unit_in[pl.ds(pl.multiple_of(source * 8, 8), 8), :] = unit_out[my_unit // 4, my_unit % 4]
        wait_units(spread_recv, 2 * chips - 1)

        def widen(s, carry):
            part = unit_in[pl.ds(pl.multiple_of(s * 8, 8), 8), :]
            for m in range(4):
                gathered[pl.ds(pl.multiple_of(s * 32 + 8 * m, 8), 8), :] = wide_roll(part, -32 * m, 1)
            return carry

        lax.fori_loop(0, 2 * chips, widen, 0, unroll=4)
        quarter = lax.broadcasted_iota(jnp.int32, (8, 128), 1) // 32

        def pack(chip, core):
            owner = 2 * chip + core
            pick(chip, core)
            total = ordered[pl.ds(pl.multiple_of(owner * 32, 32), 8), :]
            for m in (1, 2, 3):
                part = ordered[pl.ds(pl.multiple_of(owner * 32 + 8 * m, 8), 8), :]
                total = jnp.where(quarter == m, wide_roll(part, 32 * m, 1), total)
            unit_in[pl.ds(pl.multiple_of(owner * 8, 8), 8), :] = total

        def send(chip, core):
            remote(block(unit_in, 2 * chip + core, 8), unit_back.at[my_unit // 4, my_unit % 4], home_send, unit_recv, (chip, core))

        def step(k, carry):
            chip = chip_at(b, k % chips)
            pack(chip, 0)
            pack(chip, 1)

            @pl.when(k > 1)
            def _():
                before = chip_at(b, k - 1)
                send(before, 0)
                send(before, 1)

            return carry

        lax.fori_loop(1, chips + 1, step, 0)
        unit_back[my_unit // 4, my_unit % 4] = unit_in[pl.ds(pl.multiple_of(2 * b * 8, 8), 8), :]
        send(b, 1)
        wait_units(home_send, 2 * chips - 1)
        wait_rows(row_send, chips)
        wait_units(unit_send, UNITS - 1)
        wait_rows(home_recv, chips)
        wait_units(unit_recv, UNITS - 1)

    @pl.when((c == 0) & jnp.logical_not(has_unit))
    def _():
        wait_rows(row_send, chips)
        wait_units(unit_send, UNITS)
        wait_rows(home_recv, chips)
        wait_units(unit_recv, UNITS)

    back = quarters([unit_back[:, h] for h in range(4)], -1)
    for n in range(12):
        q, ih = 16 + n // 4, n % 4
        for m in range(4):
            out_ref[q, pl.ds(8 * m, 8), pl.ds(128 * ih, 128)] = back[m][n]


def kernel(chips, f_hbm, levels, plan, out_ref, *scratch):
    rows, plan_all = scratch[:2]
    drain = lbm_steps(chips, f_hbm, levels, plan, rows, plan_all, *scratch[2:16])
    migrate(chips, out_ref, rows, plan_all, *scratch[16:])
    drain()


def body(f_home, levels, plan):
    chips = lax.axis_size("blocks")
    f32, i32 = jnp.float32, jnp.int32
    dma = pltpu.SemaphoreType.DMA
    out = pl.pallas_call(
        lambda *refs: kernel(chips, *refs),
        out_shape=jax.ShapeDtypeStruct((19, 32, 512), f32),
        in_specs=[pl.BlockSpec(memory_space=pltpu.HBM)] * 3,
        out_specs=pl.BlockSpec(memory_space=pltpu.VMEM),
        scratch_shapes=[
            pltpu.VMEM((ROWS, 32, 128), f32),
            pltpu.VMEM((2 * chips, 1, 128), i32),
            pltpu.SMEM((32,), i32),
            pltpu.SMEM((32,), i32),
            pltpu.VMEM((4, 19, 32, 128), f32),
            pltpu.VMEM((19, 4, 32, 128), f32),
            pltpu.VMEM((STEPS, 2, 19, 4, 6, 8, 128), f32),
            pltpu.VMEM((19, 4, 4, 8, 128), f32),
            pltpu.VMEM((STEPS, 2, 5, 4, 8, 128), f32),
            pltpu.VMEM((STEPS, 2, 5, 6, 8, 128), f32),
            pltpu.VMEM((3, 4, 8, 128), f32),
            dma((6,)),
            dma((STEPS, 16)),
            dma((STEPS, 16)),
            dma((4,)),
            dma((4,)),
            pltpu.VMEM((128, 128), i32),
            pltpu.VMEM((128, 128), i32),
            pltpu.SMEM((128, 128), i32),
            pltpu.VMEM((64 * chips, 128), f32),
            pltpu.VMEM((64 * chips, 128), f32),
            pltpu.VMEM((12, 4, 8, 128), f32),
            pltpu.VMEM((16 * chips, 128), f32),
            pltpu.VMEM((12, 4, 8, 128), f32),
        ]
        + [dma] * 7,
        compiler_params=pltpu.CompilerParams(
            collective_id=0, has_side_effects=True, vmem_limit_bytes=VMEM_LIMIT
        ),
        name="lattice_and_owners",
    )(f_home.transpose(1, 0, 2), levels, plan)
    return out.transpose(1, 0, 2)


def solution(mesh):
    spec = P(("blocks", "cross"))
    return jax.shard_map(
        body, mesh=mesh, in_specs=(spec, spec, spec), out_specs=spec, check_vma=False
    )
```

```python
import jax
import jax.numpy as jnp
from jax import lax
from jax.experimental import pallas as pl
from jax.experimental.pallas import tpu as pltpu
from jax.sharding import PartitionSpec as P

STEPS = 2
MESH = pl.DeviceIdType.MESH
VELOCITIES = (
    (0, 0, 0),
    (1, 0, 0),
    (-1, 0, 0),
    (0, 1, 0),
    (0, -1, 0),
    (0, 0, 1),
    (0, 0, -1),
    (1, 1, 0),
    (-1, -1, 0),
    (1, -1, 0),
    (-1, 1, 0),
    (1, 0, 1),
    (-1, 0, -1),
    (1, 0, -1),
    (-1, 0, 1),
    (0, 1, 1),
    (0, -1, -1),
    (0, 1, -1),
    (0, -1, 1),
)
WEIGHTS = (1.0 / 3.0,) + (1.0 / 18.0,) * 6 + (1.0 / 36.0,) * 12
PAIRS = tuple((q, q + 1) for q in range(1, 19, 2))
X_SPEEDS = ((1, 7, 9, 11, 13), (2, 8, 10, 12, 14))
Y_SPEEDS = ((3, 7, 10, 15, 17), (4, 8, 9, 16, 18))
TAU_COARSE = 0.55
TAU_FINE = 2.0 * TAU_COARSE - 0.5
RESCALE = TAU_FINE / (2.0 * TAU_COARSE)
INFLOW = 0.08
ROWS = 76
UNITS = 48
VMEM_LIMIT = 56 * 1024 * 1024


def inflow_value(speed):
    along = VELOCITIES[speed][0] * INFLOW
    return WEIGHTS[speed] * (1.0 + 3.0 * along + 4.5 * along * along - 1.5 * INFLOW * INFLOW)


def equilibrium(field):
    density = field[0]
    for q in range(1, 19):
        density = density + field[q]
    inverse = 1.0 / density
    velocity = []
    for axis in range(3):
        total = None
        for q in range(1, 19):
            sign = VELOCITIES[q][axis]
            if sign:
                if total is None:
                    total = field[q] if sign > 0 else -field[q]
                else:
                    total = total + field[q] if sign > 0 else total - field[q]
        velocity.append(total * inverse)
    ux, uy, uz = velocity
    base = 1.0 - 1.5 * (ux * ux + uy * uy + uz * uz)
    out = [None] * 19
    out[0] = WEIGHTS[0] * density * base
    for plus, minus in PAIRS:
        along = None
        for axis in range(3):
            sign = VELOCITIES[plus][axis]
            if sign:
                term = velocity[axis]
                if along is None:
                    along = term
                else:
                    along = along + term if sign > 0 else along - term
        even = base + 4.5 * along * along
        odd = 3.0 * along
        scale = WEIGHTS[plus] * density
        out[plus] = scale * (even + odd)
        out[minus] = scale * (even - odd)
    return out


def lattice_masks(shape):
    lane = lax.broadcasted_iota(jnp.int32, shape, len(shape) - 1)
    return lane, (lane // 8) % 8, lane % 8


def wide_roll(values, shift, axis):
    shift = shift % values.shape[axis]
    return values if shift == 0 else pltpu.roll(values, shift, axis)


def shifted(main, other, q):
    ex, ey, ez = VELOCITIES[q]
    n = main.shape[0]
    lane, j, k = lattice_masks((1, 8, 128))
    if ex > 0:
        main = jnp.where(lane[None] < 64, main, other)
    elif ex < 0:
        main = jnp.where(lane[None] >= 64, main, other)
    turn = 64 if ex else 0
    here = main[:, 1:5].reshape(4 * n, 8, 128)
    if ey > 0:
        there = main[:, 0:4].reshape(4 * n, 8, 128)
        here = jnp.where(j > 0, wide_roll(here, turn + 8, 2), wide_roll(there, turn - 56, 2))
        turn = 0
    elif ey < 0:
        there = main[:, 2:6].reshape(4 * n, 8, 128)
        here = jnp.where(j < 7, wide_roll(here, turn - 8, 2), wide_roll(there, turn + 56, 2))
        turn = 0
    if ez > 0:
        over = wide_roll(wide_roll(here, 1, 1), turn - 7, 2)
        here = jnp.where(k > 0, wide_roll(here, turn + 1, 2), over)
    elif ez < 0:
        over = wide_roll(wide_roll(here, 7, 1), turn + 7, 2)
        here = jnp.where(k < 7, wide_roll(here, turn - 1, 2), over)
    else:
        here = wide_roll(here, turn, 2)
    return here.reshape(n, 4, 8, 128)


def shifted_inside(main, q):
    ex, ey, ez = VELOCITIES[q]
    shape = (4, 1, 8, 128)
    lane, j, k = lattice_masks(shape)
    high = lax.broadcasted_iota(jnp.int32, shape, 0)
    inside = lane >= 0
    if ex > 0:
        other = jnp.concatenate([main[:1], main[:3]], axis=0)
        main = jnp.where(lane < 64, main, other)
        inside = inside & (high * 128 + lane >= 64)
    elif ex < 0:
        other = jnp.concatenate([main[1:], main[3:]], axis=0)
        main = jnp.where(lane >= 64, main, other)
        inside = inside & (high * 128 + lane < 448)
    if ey:
        inside = inside & ((j > 0) if ey > 0 else (j < 7))
    if ez:
        inside = inside & ((k > 0) if ez > 0 else (k < 7))
    turn = (64 if ex else 0) + 8 * ey + ez
    moved = wide_roll(main.reshape(16, 8, 128), turn, 2)
    return moved.reshape(4, 4, 8, 128), inside


def lbm_steps(
    blocks, f_hbm, levels_hbm, plan_hbm, rows, plan_all, levels, plan, raw, state, both, work, pack_x, halo_x, coef,
    load_sem, send_sem, recv_sem, round_send, round_recv,
):
    b = lax.axis_index("blocks")
    c = lax.axis_index("cross")
    has_low, has_high = b > 0, b < blocks - 1
    low, high = jnp.maximum(b - 1, 0), jnp.minimum(b + 1, blocks - 1)

    loads = [
        pltpu.make_async_copy(
            f_hbm.at[:, :, pl.ds(128 * ih, 128)], raw.at[ih], load_sem.at[ih]
        )
        for ih in range(4)
    ]
    numbers = [
        pltpu.make_async_copy(levels_hbm, levels, load_sem.at[4]),
        pltpu.make_async_copy(plan_hbm, plan, load_sem.at[5]),
    ]
    for load in numbers + loads:
        load.start()

    barrier = pltpu.get_barrier_semaphore()

    def greet(device):
        pl.semaphore_signal(barrier, inc=1, device_id=device, device_id_type=MESH)

    greet((b, 1 - c))

    @pl.when(has_low)
    def _():
        greet((low, c))
        greet((low, 1 - c))

    @pl.when(has_high)
    def _():
        greet((high, c))
        greet((high, 1 - c))

    for load in numbers:
        load.wait()
    sublane = lax.broadcasted_iota(jnp.int32, (8, 128), 0)
    for py in range(4):
        fine = jnp.zeros((8, 128), jnp.float32)
        for pz in range(8):
            fine = jnp.where(sublane == pz, levels[py * 8 + pz].astype(jnp.float32), fine)
        is_fine = fine > 0.5
        coef[0, py] = fine
        coef[1, py] = jnp.where(is_fine, (1.0 - 1.0 / TAU_FINE) / RESCALE, 1.0 - 1.0 / TAU_COARSE)
        coef[2, py] = jnp.where(is_fine, 1.0 - 1.0 / TAU_FINE, RESCALE * (1.0 - 1.0 / TAU_COARSE))

    for step in range(STEPS):
        for side in range(2):

            @pl.when(jnp.logical_not(has_low if side == 0 else has_high))
            def _():
                for n, q in enumerate(X_SPEEDS[side]):
                    halo_x[step, side, n] = jnp.full((6, 8, 128), inflow_value(q), jnp.float32)

    plan_row = jnp.zeros((1, 128), jnp.int32)
    plan_lane = lax.broadcasted_iota(jnp.int32, (1, 128), 1)
    for p in range(32):
        plan_row = jnp.where(plan_lane == p, plan[p], plan_row)
    plan_all[64 * c + b] = plan_row

    def line(axis):
        stride = (16, 4, 1)[axis]
        at = (b // stride) % 4
        return [b + stride * ((at + k) % 4 - at) for k in (1, 2, 3)]

    for axis in range(3):
        for chip in line(axis):
            greet((chip, c))

    def plan_round(number):
        size = (1, 4, 16, 64)[number]
        part = plan_all.at[pl.ds(64 * c + (b // size) * size, size)]
        peers = [(b, 1 - c)] if number == 3 else [(chip, c) for chip in line(2 - number)]
        copies = [
            pltpu.make_async_remote_copy(
                src_ref=part,
                dst_ref=part,
                send_sem=round_send.at[number],
                recv_sem=round_recv.at[number],
                device_id=peer,
                device_id_type=MESH,
            )
            for peer in peers
        ]
        for copy in copies:
            copy.start()

    def end_round(number):
        moved = plan_all.at[pl.ds(0, (3, 12, 48, 64)[number])]
        pltpu.make_async_copy(moved, moved, round_recv.at[number]).wait()
        pltpu.make_async_copy(moved, moved, round_send.at[number]).wait()

    for load in loads:
        load.wait()

    lane = lax.broadcasted_iota(jnp.int32, (4, 8, 128), 2)
    pending = []

    def over_outer(body):
        def at(pos, carry):
            body(3 * (pos // 4), pos % 4)
            return carry

        lax.fori_loop(0, 8, at, 0)

    def over_inner(body):
        def at(pos, carry):
            body(1 + pos // 4, pos % 4)
            return carry

        lax.fori_loop(0, 8, at, 0)

    for step in range(STEPS):

        def relax_both(ih, py):
            rows_of_py = pl.ds(pl.multiple_of(py * 8, 8), 8)
            if step:
                field = [state[q, ih, rows_of_py, :] for q in range(19)]
            else:
                field = [raw[ih, q, rows_of_py, :] for q in range(19)]
            balance = equilibrium(field)
            for_coarse, for_fine = coef[1, py], coef[2, py]
            for q in range(19):
                away = field[q] - balance[q]
                both[step, 0, q, ih, py + 1] = balance[q] + for_coarse * away
                both[step, 1, q, ih, py + 1] = balance[q] + for_fine * away

        over_outer(relax_both)

        copies = []

        def add(src, dst, device, send_if, recv_if):
            index = len(copies)
            copy = pltpu.make_async_remote_copy(
                src_ref=src,
                dst_ref=dst,
                send_sem=send_sem.at[step, index],
                recv_sem=recv_sem.at[step, index],
                device_id=device,
                device_id_type=MESH,
            )
            copies.append((send_if, recv_if, copy))

        for side in range(2):
            edge = 3 if side == 0 else 0
            for n, q in enumerate(X_SPEEDS[side]):
                first = both[step, 0, q, edge, 1:5]
                second = pltpu.roll(both[step, 1, q, edge, 1:5], 64, 2)
                keep = lane >= 64 if side == 0 else lane < 64
                pack_x[step, side, n] = jnp.where(keep, first, second)
        if step == 0:
            pl.semaphore_wait(
                barrier, 10 + 2 * has_low.astype(jnp.int32) + 2 * has_high.astype(jnp.int32)
            )
        for side in range(2):
            target = high if side == 0 else low
            send_if, recv_if = (has_high, has_low) if side == 0 else (has_low, has_high)
            add(
                pack_x.at[step, side],
                halo_x.at[step, side, :, pl.ds(1, 4)],
                (target, c),
                send_if,
                recv_if,
            )
            for n, q in enumerate(X_SPEEDS[side]):
                ey = VELOCITIES[q][1]
                if ey:
                    py, slot = (3, 0) if ey > 0 else (0, 5)
                    add(
                        pack_x.at[step, side, n, py],
                        halo_x.at[step, side, n, slot],
                        (target, 1 - c),
                        send_if,
                        recv_if,
                    )
        def start(chosen):
            for send_if, recv_if, copy in chosen:
                if send_if is None:
                    copy.start()
                else:
                    pl.when(send_if)(copy.start)

        def arrive(chosen):
            for send_if, recv_if, copy in chosen:
                if recv_if is None:
                    copy.wait_recv()
                else:
                    pl.when(recv_if)(copy.wait_recv)

        start(copies)
        along_x = len(copies)
        over_inner(relax_both)
        for side in range(2):
            py, slot = (4, 0) if side == 0 else (1, 5)
            for q in Y_SPEEDS[side]:
                add(
                    both.at[step, :, q, :, py],
                    both.at[step, :, q, :, slot],
                    (b, 1 - c),
                    None,
                    None,
                )
        start(copies[along_x:])
        if step == 0:
            plan_round(0)
        else:
            end_round(1)
            plan_round(2)
        fine = coef[0] > 0.5

        def stream(q, first, last, halo):
            ex = VELOCITIES[q][0]
            result = []
            for kind in range(2):
                other = None
                if halo:
                    side = 0 if ex > 0 else 1
                    other = halo_x[step, side, X_SPEEDS[side].index(q)]
                    other = (pltpu.roll(other, 64, 2) if kind else other)[None]
                elif ex:
                    other = both[step, kind, q, first - ex : last - ex]
                result.append(shifted(both[step, kind, q, first:last], other, q))
            moved = jnp.where(fine[None], result[1], result[0])
            state[q, first:last] = moved.reshape(last - first, 32, 128)

        arrive(copies[along_x:])
        for q in range(19):
            ex = VELOCITIES[q][0]
            stream(q, 1 if ex > 0 else 0, 3 if ex < 0 else 4, False)

        def relax_again(ih, py):
            rows_of_py = pl.ds(pl.multiple_of(py * 8, 8), 8)
            field = [state[q, ih, rows_of_py, :] for q in range(19)]
            balance = equilibrium(field)
            for q in range(19):
                work[q, ih, py] = field[q] + (1.0 / TAU_FINE) * (balance[q] - field[q])

        over_inner(relax_again)
        arrive(copies[:along_x])
        pending += copies
        if step == 0:
            end_round(0)
            plan_round(1)
        else:
            end_round(2)
            plan_round(3)
        for side in range(2):
            for q in X_SPEEDS[side]:
                stream(q, 3 * side, 3 * side + 1, True)
        over_outer(relax_again)
        for q in range(19):
            moved, inside = shifted_inside(work[q], q)
            kept = state[q].reshape(4, 4, 8, 128)
            result = jnp.where(inside & fine[None], moved, kept).reshape(4, 32, 128)
            if step == STEPS - 1:
                rows[pl.ds(4 * q, 4)] = result
            else:
                state[q] = result

    end_round(3)

    def drain():
        for send_if, recv_if, copy in pending:
            if send_if is None:
                copy.wait_send()
            else:
                pl.when(send_if)(copy.wait_send)

    return drain


def spare_unit(b):
    place = (b // 16 + (b // 4) % 4 + b % 4) % 4
    return jnp.minimum((b // 4) * 3 + place, UNITS - 1), place < 3


def chip_at(b, k):
    dx = k % 4
    dz = (dx + k // 4) % 4
    dy = (dz + k // 16) % 4
    return 16 * ((b // 16 + dx) % 4) + 4 * (((b // 4) % 4 + dz) % 4) + (b % 4 + dy) % 4


def quarters(parts, sign):
    quarter = lax.broadcasted_iota(jnp.int32, parts[0].shape, parts[0].ndim - 1) // 32
    out = []
    for h in range(4):
        total = parts[h]
        for m in range(4):
            if m != h:
                total = jnp.where(quarter == m, wide_roll(parts[m], 32 * (m - h), total.ndim - 1), total)
        out.append(total)
    return out


def migrate(
    chips, out_ref, rows, plan_all, plan_turned, inv_vec, inv_smem, gathered, ordered, unit_out, unit_in, unit_back,
    local_sem, row_send, unit_send, spread_recv, home_send, home_recv, unit_recv,
):
    b = lax.axis_index("blocks")
    c = lax.axis_index("cross")
    source = 64 * c + b
    my_unit, has_unit = spare_unit(b)
    is_spare = (c == 0) & has_unit
    is_main = c == 1

    def remote(src, dst, send, recv, device):
        pltpu.make_async_remote_copy(
            src_ref=src, dst_ref=dst, send_sem=send, recv_sem=recv, device_id=device, device_id_type=MESH
        ).start()

    def block(ref, index, size):
        return ref.at[pl.ds(pl.multiple_of(index * size, size), size)]

    spare_rows = rows[pl.ds(64, 12)].reshape(12, 4, 8, 128)
    for h, part in enumerate(quarters([spare_rows[:, m] for m in range(4)], 1)):
        unit_out[:, h] = part

    def spread(k, carry):
        chip = chip_at(b, k)

        @pl.when((k > 0) | (c == 0))
        def _():
            remote(rows.at[chip], block(gathered, source, 32), row_send, spread_recv, (chip, 1))

        unit, wanted = spare_unit(chip)

        @pl.when(wanted & ((k > 0) | (c == 1)))
        def _():
            remote(unit_out.at[unit // 4, unit % 4], block(unit_in, source, 8), unit_send, spread_recv, (chip, 0))

        return carry

    lax.fori_loop(0, chips, spread, 0)

    def wait_rows(sem, count):
        part = gathered.at[pl.ds(0, 32 * count)]
        pltpu.make_async_copy(part, part, sem).wait()

    def wait_units(sem, count):
        part = unit_in.at[pl.ds(0, 8 * count)]
        pltpu.make_async_copy(part, part, sem).wait()

    def find_slots():
        plans = plan_all[:, 0, :]
        plan_turned[...] = plans.T
        sub = lax.broadcasted_iota(jnp.int32, (128, 128), 0)
        lane = lax.broadcasted_iota(jnp.int32, (128, 128), 1)

        def place(p, carry):
            plans, total = carry
            owner = plan_turned[pl.ds(p, 1), :] // 32
            hot = jnp.where(owner == sub, 1.0, 0.0)
            slot = plans[:, 0:1] % 32
            value = jnp.where(slot == lane, sub, jnp.where(slot + 32 == lane, p, 0))
            total = total + jnp.dot(
                hot.astype(jnp.bfloat16),
                value.astype(jnp.float32).astype(jnp.bfloat16),
                preferred_element_type=jnp.float32,
            )
            return pltpu.roll(plans, 127, 1), total

        _, total = lax.fori_loop(0, 32, place, (plans, jnp.zeros((128, 128), jnp.float32)))
        total = total.astype(jnp.int32)
        inv_vec[...] = jnp.clip(total * 32 + pltpu.roll(total, 96, 1), 0, 64 * chips - 1)
        move = pltpu.make_async_copy(inv_vec, inv_smem, local_sem)
        move.start()
        move.wait()

    def pick(chip, core):
        owner = 2 * chip + core
        for u in range(32):
            index = inv_smem[owner, u]
            ordered[pl.ds(owner * 32 + u, 1), :] = gathered[pl.ds(index, 1), :]

    my_place = out_ref.at[b // 4, :, pl.ds(pl.multiple_of((b % 4) * 128, 128), 128)]

    @pl.when(is_main)
    def _():
        find_slots()
        gathered[pl.ds(pl.multiple_of(source * 32, 32), 32), :] = rows[b]
        wait_rows(spread_recv, 2 * chips - 1)

        def send(chip, core):
            remote(block(ordered, 2 * chip + core, 32), my_place, home_send, home_recv, (chip, core))

        def step(k, carry):
            chip = chip_at(b, k % chips)
            pick(chip, 0)
            pick(chip, 1)

            @pl.when(k > 1)
            def _():
                before = chip_at(b, k - 1)
                send(before, 0)
                send(before, 1)

            return carry

        lax.fori_loop(1, chips + 1, step, 0)
        out_ref[b // 4, :, pl.ds(pl.multiple_of((b % 4) * 128, 128), 128)] = ordered[
            pl.ds(pl.multiple_of((2 * b + 1) * 32, 32), 32), :
        ]
        send(b, 0)
        wait_rows(home_send, 2 * chips - 1)
        wait_rows(row_send, chips - 1)
        wait_units(unit_send, UNITS)
        wait_rows(home_recv, chips - 1)
        wait_units(unit_recv, UNITS)

    @pl.when(is_spare)
    def _():
        find_slots()
        unit_in[pl.ds(pl.multiple_of(source * 8, 8), 8), :] = unit_out[my_unit // 4, my_unit % 4]
        wait_units(spread_recv, 2 * chips - 1)

        def widen(s, carry):
            part = unit_in[pl.ds(pl.multiple_of(s * 8, 8), 8), :]
            for m in range(4):
                gathered[pl.ds(pl.multiple_of(s * 32 + 8 * m, 8), 8), :] = wide_roll(part, -32 * m, 1)
            return carry

        lax.fori_loop(0, 2 * chips, widen, 0, unroll=4)
        quarter = lax.broadcasted_iota(jnp.int32, (8, 128), 1) // 32

        def pack(chip, core):
            owner = 2 * chip + core
            pick(chip, core)
            total = ordered[pl.ds(pl.multiple_of(owner * 32, 32), 8), :]
            for m in (1, 2, 3):
                part = ordered[pl.ds(pl.multiple_of(owner * 32 + 8 * m, 8), 8), :]
                total = jnp.where(quarter == m, wide_roll(part, 32 * m, 1), total)
            unit_in[pl.ds(pl.multiple_of(owner * 8, 8), 8), :] = total

        def send(chip, core):
            remote(block(unit_in, 2 * chip + core, 8), unit_back.at[my_unit // 4, my_unit % 4], home_send, unit_recv, (chip, core))

        def step(k, carry):
            chip = chip_at(b, k % chips)
            pack(chip, 0)
            pack(chip, 1)

            @pl.when(k > 1)
            def _():
                before = chip_at(b, k - 1)
                send(before, 0)
                send(before, 1)

            return carry

        lax.fori_loop(1, chips + 1, step, 0)
        unit_back[my_unit // 4, my_unit % 4] = unit_in[pl.ds(pl.multiple_of(2 * b * 8, 8), 8), :]
        send(b, 1)
        wait_units(home_send, 2 * chips - 1)
        wait_rows(row_send, chips)
        wait_units(unit_send, UNITS - 1)
        wait_rows(home_recv, chips)
        wait_units(unit_recv, UNITS - 1)

    @pl.when((c == 0) & jnp.logical_not(has_unit))
    def _():
        wait_rows(row_send, chips)
        wait_units(unit_send, UNITS)
        wait_rows(home_recv, chips)
        wait_units(unit_recv, UNITS)

    back = quarters([unit_back[:, h] for h in range(4)], -1)
    for n in range(12):
        q, ih = 16 + n // 4, n % 4
        for m in range(4):
            out_ref[q, pl.ds(8 * m, 8), pl.ds(128 * ih, 128)] = back[m][n]


def kernel(chips, f_hbm, levels, plan, out_ref, *scratch):
    rows, plan_all = scratch[:2]
    drain = lbm_steps(chips, f_hbm, levels, plan, rows, plan_all, *scratch[2:16])
    migrate(chips, out_ref, rows, plan_all, *scratch[16:])
    drain()


def body(f_home, levels, plan):
    chips = lax.axis_size("blocks")
    f32, i32 = jnp.float32, jnp.int32
    dma = pltpu.SemaphoreType.DMA
    out = pl.pallas_call(
        lambda *refs: kernel(chips, *refs),
        out_shape=pltpu.VMEM((19, 32, 512), f32),
        in_specs=[pl.BlockSpec(memory_space=pltpu.HBM)] * 3,
        out_specs=pl.BlockSpec(memory_space=pltpu.VMEM),
        scratch_shapes=[
            pltpu.VMEM((ROWS, 32, 128), f32),
            pltpu.VMEM((2 * chips, 1, 128), i32),
            pltpu.SMEM((32,), i32),
            pltpu.SMEM((32,), i32),
            pltpu.VMEM((4, 19, 32, 128), f32),
            pltpu.VMEM((19, 4, 32, 128), f32),
            pltpu.VMEM((STEPS, 2, 19, 4, 6, 8, 128), f32),
            pltpu.VMEM((19, 4, 4, 8, 128), f32),
            pltpu.VMEM((STEPS, 2, 5, 4, 8, 128), f32),
            pltpu.VMEM((STEPS, 2, 5, 6, 8, 128), f32),
            pltpu.VMEM((3, 4, 8, 128), f32),
            dma((6,)),
            dma((STEPS, 16)),
            dma((STEPS, 16)),
            dma((4,)),
            dma((4,)),
            pltpu.VMEM((128, 128), i32),
            pltpu.VMEM((128, 128), i32),
            pltpu.SMEM((128, 128), i32),
            pltpu.VMEM((64 * chips, 128), f32),
            pltpu.VMEM((64 * chips, 128), f32),
            pltpu.VMEM((12, 4, 8, 128), f32),
            pltpu.VMEM((16 * chips, 128), f32),
            pltpu.VMEM((12, 4, 8, 128), f32),
        ]
        + [dma] * 7,
        compiler_params=pltpu.CompilerParams(
            collective_id=0, has_side_effects=True, vmem_limit_bytes=VMEM_LIMIT
        ),
        name="lattice_and_owners",
    )(f_home.transpose(1, 0, 2), levels, plan)
    return out.transpose(1, 0, 2)


def solution(mesh):
    spec = P(("blocks", "cross"))
    return jax.shard_map(
        body, mesh=mesh, in_specs=(spec, spec, spec), out_specs=spec, check_vma=False
    )
```

```python
import jax
import jax.numpy as jnp
from jax import lax
from jax.experimental import pallas as pl
from jax.experimental.pallas import tpu as pltpu
from jax.sharding import PartitionSpec as P

STEPS = 2
MESH = pl.DeviceIdType.MESH
VELOCITIES = (
    (0, 0, 0),
    (1, 0, 0),
    (-1, 0, 0),
    (0, 1, 0),
    (0, -1, 0),
    (0, 0, 1),
    (0, 0, -1),
    (1, 1, 0),
    (-1, -1, 0),
    (1, -1, 0),
    (-1, 1, 0),
    (1, 0, 1),
    (-1, 0, -1),
    (1, 0, -1),
    (-1, 0, 1),
    (0, 1, 1),
    (0, -1, -1),
    (0, 1, -1),
    (0, -1, 1),
)
WEIGHTS = (1.0 / 3.0,) + (1.0 / 18.0,) * 6 + (1.0 / 36.0,) * 12
PAIRS = tuple((q, q + 1) for q in range(1, 19, 2))
X_SPEEDS = ((1, 7, 9, 11, 13), (2, 8, 10, 12, 14))
Y_SPEEDS = ((3, 7, 10, 15, 17), (4, 8, 9, 16, 18))
TAU_COARSE = 0.55
TAU_FINE = 2.0 * TAU_COARSE - 0.5
RESCALE = TAU_FINE / (2.0 * TAU_COARSE)
INFLOW = 0.08


def row_units():
    early, late = [], []
    for q in range(19):
        for ih in range(4):
            ready = ((1, 2), (2,), (1,))[VELOCITIES[q][0]]
            (early if ih in ready else late).append((q, ih))
    chips = []
    for b in range(64):
        x, z, y = b // 16, b // 4 % 4, b % 4
        if (x + z) % 2 or y != (x + z) % 4:
            chips.append(b)
    units = {}
    for n, row in enumerate(early):
        units[row] = ("early", chips[2 * n : 2 * n + 2])
    for n, row in enumerate(late):
        units[row] = ("late", n)
    return units


UNITS = row_units()
EARLY = 56
VMEM_LIMIT = 56 * 1024 * 1024


def has_early(b):
    x, z, y = b // 16, (b // 4) % 4, b % 4
    return ((x + z) % 2 == 1) | (y != (x + z) % 4)


def inflow_value(speed):
    along = VELOCITIES[speed][0] * INFLOW
    return WEIGHTS[speed] * (1.0 + 3.0 * along + 4.5 * along * along - 1.5 * INFLOW * INFLOW)


def equilibrium(field):
    density = field[0]
    for q in range(1, 19):
        density = density + field[q]
    inverse = 1.0 / density
    velocity = []
    for axis in range(3):
        total = None
        for q in range(1, 19):
            sign = VELOCITIES[q][axis]
            if sign:
                if total is None:
                    total = field[q] if sign > 0 else -field[q]
                else:
                    total = total + field[q] if sign > 0 else total - field[q]
        velocity.append(total * inverse)
    ux, uy, uz = velocity
    base = 1.0 - 1.5 * (ux * ux + uy * uy + uz * uz)
    out = [None] * 19
    out[0] = WEIGHTS[0] * density * base
    for plus, minus in PAIRS:
        along = None
        for axis in range(3):
            sign = VELOCITIES[plus][axis]
            if sign:
                term = velocity[axis]
                if along is None:
                    along = term
                else:
                    along = along + term if sign > 0 else along - term
        even = base + 4.5 * along * along
        odd = 3.0 * along
        scale = WEIGHTS[plus] * density
        out[plus] = scale * (even + odd)
        out[minus] = scale * (even - odd)
    return out


def lattice_masks(shape):
    lane = lax.broadcasted_iota(jnp.int32, shape, len(shape) - 1)
    return lane, (lane // 8) % 8, lane % 8


def wide_roll(values, shift, axis):
    shift = shift % values.shape[axis]
    return values if shift == 0 else pltpu.roll(values, shift, axis)


def shifted(main, other, q):
    ex, ey, ez = VELOCITIES[q]
    n = main.shape[0]
    lane, j, k = lattice_masks((1, 8, 128))
    if ex > 0:
        main = jnp.where(lane[None] < 64, main, other)
    elif ex < 0:
        main = jnp.where(lane[None] >= 64, main, other)
    turn = 64 if ex else 0
    here = main[:, 1:5].reshape(4 * n, 8, 128)
    if ey > 0:
        there = main[:, 0:4].reshape(4 * n, 8, 128)
        here = jnp.where(j > 0, wide_roll(here, turn + 8, 2), wide_roll(there, turn - 56, 2))
        turn = 0
    elif ey < 0:
        there = main[:, 2:6].reshape(4 * n, 8, 128)
        here = jnp.where(j < 7, wide_roll(here, turn - 8, 2), wide_roll(there, turn + 56, 2))
        turn = 0
    if ez > 0:
        over = wide_roll(wide_roll(here, 1, 1), turn - 7, 2)
        here = jnp.where(k > 0, wide_roll(here, turn + 1, 2), over)
    elif ez < 0:
        over = wide_roll(wide_roll(here, 7, 1), turn + 7, 2)
        here = jnp.where(k < 7, wide_roll(here, turn - 1, 2), over)
    else:
        here = wide_roll(here, turn, 2)
    return here.reshape(n, 4, 8, 128)


def lane_blocks(parts):
    n = len(parts)
    section = lax.broadcasted_iota(jnp.int32, parts[0].shape, parts[0].ndim - 1) // (128 // n)
    out = []
    for h in range(n):
        total = parts[h]
        for m in range(n):
            if m != h:
                total = jnp.where(section == m, wide_roll(parts[m], 128 // n * (m - h), total.ndim - 1), total)
        out.append(total)
    return out


def chosen(parts):
    section = lax.broadcasted_iota(jnp.int32, (8, 128), 1) // 32
    total = None
    for h, (part, at) in enumerate(parts):
        part = wide_roll(part, 32 * (h - at), 1)
        total = part if total is None else jnp.where(section == h, part, total)
    return total


def shifted_inside(work, q, ih):
    ex, ey, ez = VELOCITIES[q]
    lane, j, k = lattice_masks((1, 8, 128))
    main = work[q, ih]
    inside = None

    def both_of(first, second):
        return second if first is None else first & second

    if ex:
        low = lane < 64
        if 0 <= ih - ex < 4:
            main = jnp.where(low if ex > 0 else ~low, main, work[q, ih - ex])
        else:
            inside = ~low if ex > 0 else low
    if ey:
        inside = both_of(inside, (j > 0) if ey > 0 else (j < 7))
    if ez:
        inside = both_of(inside, (k > 0) if ez > 0 else (k < 7))
    return wide_roll(main, (64 if ex else 0) + 8 * ey + ez, 2), inside


def lbm_steps(
    blocks, f_hbm, levels_hbm, plan_hbm, sends, late_rows, plan_all, levels, plan, raw, state, both, work, pack_x, halo_x, coef,
    load_sem, send_sem, recv_sem, round_send, round_recv, ready, send_early,
):
    b = lax.axis_index("blocks")
    c = lax.axis_index("cross")
    has_low, has_high = b > 0, b < blocks - 1
    low, high = jnp.maximum(b - 1, 0), jnp.minimum(b + 1, blocks - 1)

    loads = [
        pltpu.make_async_copy(
            f_hbm.at[:, :, pl.ds(128 * ih, 128)], raw.at[ih], load_sem.at[ih]
        )
        for ih in range(4)
    ]
    numbers = [
        pltpu.make_async_copy(levels_hbm, levels, load_sem.at[4]),
        pltpu.make_async_copy(plan_hbm, plan, load_sem.at[5]),
    ]
    for load in numbers + loads:
        load.start()

    barrier = pltpu.get_barrier_semaphore()

    def greet(device):
        pl.semaphore_signal(barrier, inc=1, device_id=device, device_id_type=MESH)

    greet((b, 1 - c))

    def line(axis):
        stride = (16, 4, 1)[axis]
        at = (b // stride) % 4
        return [b + stride * ((at + k) % 4 - at) for k in (1, 2, 3)]

    for axis in range(3):
        for chip in line(axis):
            greet((chip, c))

    @pl.when(has_low)
    def _():
        greet((low, c))
        greet((low, 1 - c))

    @pl.when(has_high)
    def _():
        greet((high, c))
        greet((high, 1 - c))

    for load in numbers:
        load.wait()
    sublane = lax.broadcasted_iota(jnp.int32, (8, 128), 0)
    for py in range(4):
        fine = jnp.zeros((8, 128), jnp.float32)
        for pz in range(8):
            fine = jnp.where(sublane == pz, levels[py * 8 + pz].astype(jnp.float32), fine)
        is_fine = fine > 0.5
        coef[0, py] = fine
        coef[1, py] = jnp.where(is_fine, (1.0 - 1.0 / TAU_FINE) / RESCALE, 1.0 - 1.0 / TAU_COARSE)
        coef[2, py] = jnp.where(is_fine, 1.0 - 1.0 / TAU_FINE, RESCALE * (1.0 - 1.0 / TAU_COARSE))

    for step in range(STEPS):
        for side in range(2):

            @pl.when(jnp.logical_not(has_low if side == 0 else has_high))
            def _():
                for n, q in enumerate(X_SPEEDS[side]):
                    halo_x[step, side, n] = jnp.full((6, 8, 128), inflow_value(q), jnp.float32)

    plan_row = jnp.zeros((1, 128), jnp.int32)
    plan_lane = lax.broadcasted_iota(jnp.int32, (1, 128), 1)
    for p in range(32):
        plan_row = jnp.where(plan_lane == p, plan[p], plan_row)
    plan_all[64 * c + b] = plan_row

    def plan_round(number):
        size = (1, 4, 16, 64)[number]
        part = plan_all.at[pl.ds(64 * c + (b // size) * size, size)]
        peers = [(b, 1 - c)] if number == 3 else [(chip, c) for chip in line(2 - number)]
        copies = [
            pltpu.make_async_remote_copy(
                src_ref=part,
                dst_ref=part,
                send_sem=round_send.at[number],
                recv_sem=round_recv.at[number],
                device_id=peer,
                device_id_type=MESH,
            )
            for peer in peers
        ]
        for copy in copies:
            copy.start()

    def end_round(number):
        moved = plan_all.at[pl.ds(0, (3, 12, 48, 64)[number])]
        pltpu.make_async_copy(moved, moved, round_recv.at[number]).wait()
        pltpu.make_async_copy(moved, moved, round_send.at[number]).wait()

    for load in loads:
        load.wait()

    lane = lax.broadcasted_iota(jnp.int32, (4, 8, 128), 2)
    pending = []

    def over_outer(body):
        def at(pos, carry):
            body(3 * (pos // 4), pos % 4)
            return carry

        lax.fori_loop(0, 8, at, 0)

    def over_inner(body):
        def at(pos, carry):
            body(1 + pos // 4, pos % 4)
            return carry

        lax.fori_loop(0, 8, at, 0)

    for step in range(STEPS):

        def relax_both(ih, py):
            rows_of_py = pl.ds(pl.multiple_of(py * 8, 8), 8)
            if step:
                field = [state[q, ih, rows_of_py, :] for q in range(19)]
            else:
                field = [raw[ih, q, rows_of_py, :] for q in range(19)]
            balance = equilibrium(field)
            for_coarse, for_fine = coef[1, py], coef[2, py]
            for q in range(19):
                away = field[q] - balance[q]
                both[step, 0, q, ih, py + 1] = balance[q] + for_coarse * away
                both[step, 1, q, ih, py + 1] = balance[q] + for_fine * away

        over_outer(relax_both)

        copies = []

        def add(src, dst, device, send_if, recv_if):
            index = len(copies)
            copy = pltpu.make_async_remote_copy(
                src_ref=src,
                dst_ref=dst,
                send_sem=send_sem.at[step, index],
                recv_sem=recv_sem.at[step, index],
                device_id=device,
                device_id_type=MESH,
            )
            copies.append((send_if, recv_if, copy))

        for side in range(2):
            edge = 3 if side == 0 else 0
            for n, q in enumerate(X_SPEEDS[side]):
                first = both[step, 0, q, edge, 1:5]
                second = pltpu.roll(both[step, 1, q, edge, 1:5], 64, 2)
                keep = lane >= 64 if side == 0 else lane < 64
                pack_x[step, side, n] = jnp.where(keep, first, second)
        if step == 0:
            pl.semaphore_wait(
                barrier, 10 + 2 * has_low.astype(jnp.int32) + 2 * has_high.astype(jnp.int32)
            )
            for chip in line(2):
                pl.semaphore_signal(ready.at[0], inc=1, device_id=(chip, c), device_id_type=MESH)
        for side in range(2):
            target = high if side == 0 else low
            send_if, recv_if = (has_high, has_low) if side == 0 else (has_low, has_high)
            add(
                pack_x.at[step, side],
                halo_x.at[step, side, :, pl.ds(1, 4)],
                (target, c),
                send_if,
                recv_if,
            )
            for n, q in enumerate(X_SPEEDS[side]):
                ey = VELOCITIES[q][1]
                if ey:
                    py, slot = (3, 0) if ey > 0 else (0, 5)
                    add(
                        pack_x.at[step, side, n, py],
                        halo_x.at[step, side, n, slot],
                        (target, 1 - c),
                        send_if,
                        recv_if,
                    )
        def start(chosen):
            for send_if, recv_if, copy in chosen:
                if send_if is None:
                    copy.start()
                else:
                    pl.when(send_if)(copy.start)

        def arrive(chosen):
            for send_if, recv_if, copy in chosen:
                if recv_if is None:
                    copy.wait_recv()
                else:
                    pl.when(recv_if)(copy.wait_recv)

        start(copies)
        along_x = len(copies)
        over_inner(relax_both)
        for side in range(2):
            py, slot = (4, 0) if side == 0 else (1, 5)
            for q in Y_SPEEDS[side]:
                add(
                    both.at[step, :, q, :, py],
                    both.at[step, :, q, :, slot],
                    (b, 1 - c),
                    None,
                    None,
                )
        start(copies[along_x:])
        if step == 0:
            plan_round(0)
        else:
            end_round(1)
            plan_round(2)
        fine = coef[0]

        def stream(q, first, last, halo):
            ex = VELOCITIES[q][0]
            result = []
            for kind in range(2):
                other = None
                if halo:
                    side = 0 if ex > 0 else 1
                    other = halo_x[step, side, X_SPEEDS[side].index(q)]
                    other = (pltpu.roll(other, 64, 2) if kind else other)[None]
                elif ex:
                    other = both[step, kind, q, first - ex : last - ex]
                result.append(shifted(both[step, kind, q, first:last], other, q))
            moved = jnp.where(fine[None] > 0.5, result[1], result[0])
            state[q, first:last] = moved.reshape(last - first, 32, 128)

        arrive(copies[along_x:])
        for q in range(19):
            ex = VELOCITIES[q][0]
            stream(q, 1 if ex > 0 else 0, 3 if ex < 0 else 4, False)

        def relax_again(ih, py):
            rows_of_py = pl.ds(pl.multiple_of(py * 8, 8), 8)
            field = [state[q, ih, rows_of_py, :] for q in range(19)]
            balance = equilibrium(field)
            for q in range(19):
                work[q, ih, py] = field[q] + (1.0 / TAU_FINE) * (balance[q] - field[q])

        def finish(q, ih):
            moved, inside = shifted_inside(work, q, ih)
            inside = fine > 0.5 if inside is None else inside & (fine > 0.5)
            result = jnp.where(inside, moved, state[q, ih].reshape(4, 8, 128)).reshape(32, 128)
            if step == STEPS - 1:
                kind, place = UNITS[q, ih]
                if kind == "late":
                    late_rows[place] = result
                else:
                    for chip, block in zip(place, lane_blocks([result[:16], result[16:]])):
                        sends[kind][chip] = block
            else:
                state[q, ih] = result

        if step == 0:
            pl.semaphore_wait(ready.at[0], 3)
            for chip in line(1):
                pl.semaphore_signal(ready.at[1], inc=1, device_id=(chip, c), device_id_type=MESH)
        over_inner(relax_again)
        last = step == STEPS - 1
        early = [row for row, unit in UNITS.items() if unit[0] == "early"]
        if last:
            for q, ih in early:
                finish(q, ih)
            pl.semaphore_wait(ready.at[2], 1)
            send_early()
        arrive(copies[:along_x])
        pending += copies
        if step == 0:
            end_round(0)
            plan_round(1)
            pl.semaphore_wait(ready.at[1], 3)
            pl.semaphore_signal(ready.at[2], inc=1, device_id=(b, 1 - c), device_id_type=MESH)
        else:
            end_round(2)
            plan_round(3)
        for side in range(2):
            for q in X_SPEEDS[side]:
                stream(q, 3 * side, 3 * side + 1, True)
        over_outer(relax_again)
        for q in range(19):
            for ih in range(4):
                if not (last and (q, ih) in early):
                    finish(q, ih)

    def drain():
        for send_if, recv_if, copy in pending:
            if send_if is None:
                copy.wait_send()
            else:
                pl.when(send_if)(copy.wait_send)

    return drain, lambda: end_round(3)


def chip_at(b, k):
    def mod(value):
        return lax.rem(value, jnp.int32(4))

    def div(value, by):
        return lax.div(value, jnp.int32(by))

    dx = mod(k)
    dz = dx + div(k, 4)
    dy = dz + div(k, 16)
    return 16 * mod(div(b, 16) + dx) + 4 * mod(div(b, 4) + dz) + mod(b + dy)


def migrate(chips, sends, late_rows, plan_all, homes, plan_turned, inv_vec, inv_smem, wide, ordered, outs, local_sem, sems):
    b = lax.axis_index("blocks")
    c = lax.axis_index("cross")
    source = 64 * c + b
    cores = {"early": 1, "late": 0}
    sizes = {"early": 16, "late": 24}

    def remote(src, dst, send, recv, device):
        pltpu.make_async_remote_copy(
            src_ref=src, dst_ref=dst, send_sem=send, recv_sem=recv, device_id=device, device_id_type=MESH
        ).start()

    def wait_for(kind, sem, count):
        part = wide.at[pl.ds(0, sizes[kind] * count)]
        pltpu.make_async_copy(part, part, sems.at[sem]).wait()

    number = {"early": 0, "late": 4}

    def spread(kind, chip, k):
        @pl.when((k > 0) | (c != cores[kind]))
        def _():
            n = number[kind]
            land = wide.at[pl.ds(pl.multiple_of(source * 32, 32), sizes[kind])]
            remote(sends[kind].at[chip], land, sems.at[n], sems.at[n + 1], (chip, cores[kind]))

    def send_early():
        def step(k, carry):
            chip = chip_at(b, k)
            pl.when(has_early(chip))(lambda: spread("early", chip, k))
            return carry

        lax.fori_loop(0, chips, step, 0)

    end_plan = yield send_early

    for chip in range(64):
        columns = [divmod(3 * chip + i, 4) for i in range(3)]
        for m in range(3):
            parts = [(late_rows[n, 8 * m : 8 * m + 8], h) for n, h in columns]
            n, h = columns[m]
            sends["late"][chip, 8 * m : 8 * m + 8] = chosen(parts + [(late_rows[n, 24:32], h)])

    def send_late(k, carry):
        chip = chip_at(b, k)
        spread("late", chip, k)
        return carry

    lax.fori_loop(0, chips, send_late, 0)
    end_plan()

    plans = plan_all[:, 0, :]
    plan_turned[...] = plans.T
    sub = lax.broadcasted_iota(jnp.int32, (128, 128), 0)
    lane = lax.broadcasted_iota(jnp.int32, (128, 128), 1)

    def place(p, carry):
        plans, total = carry
        owner = plan_turned[pl.ds(p, 1), :] // 32
        hot = jnp.where(owner == sub, 1.0, 0.0)
        slot = plans[:, 0:1] % 32
        value = jnp.where(slot == lane, sub, jnp.where(slot + 32 == lane, p, 0))
        total = total + jnp.dot(
            hot.astype(jnp.bfloat16),
            value.astype(jnp.float32).astype(jnp.bfloat16),
            preferred_element_type=jnp.float32,
        )
        return pltpu.roll(plans, 127, 1), total

    _, total = lax.fori_loop(0, 32, place, (plans, jnp.zeros((128, 128), jnp.float32)), unroll=4)
    total = total.astype(jnp.int32)
    inv_vec[...] = jnp.clip(total * 32 + pltpu.roll(total, 96, 1), 0, 64 * chips - 1)
    move = pltpu.make_async_copy(inv_vec, inv_smem, local_sem)
    move.start()
    move.wait()

    def serve(kind):
        out, size, n = outs[kind], sizes[kind], number[kind]
        core = cores[kind]
        wide[pl.ds(pl.multiple_of(source * 32, 32), size), :] = sends[kind][b]
        wait_for(kind, n + 1, 2 * chips - 1)
        section = lax.broadcasted_iota(jnp.int32, (8, 128), 1) // 32

        def widen(s, carry):
            at = lambda m: pl.ds(pl.multiple_of(s * 32 + 8 * m, 8), 8)
            if kind == "early":
                for m in range(2):
                    wide[at(2 + m), :] = wide_roll(wide[at(m), :], 64, 1)
            else:
                wide[at(3), :] = chosen([(wide[at(m), :], 3) for m in range(3)])
            return carry

        lax.fori_loop(0, 2 * chips, widen, 0, unroll=8)

        def pick(chip, target_core):
            owner = 2 * chip + target_core
            for u in range(32):
                index = inv_smem[owner, u]
                ordered[pl.ds(owner * 32 + u, 1), :] = wide[pl.ds(index, 1), :]
            blocks = [ordered[pl.ds(pl.multiple_of(owner * 32 + 8 * m, 8), 8), :] for m in range(4)]
            if kind == "early":
                for m in range(2):
                    out[owner, 8 * m : 8 * m + 8] = jnp.where(
                        section < 2, blocks[m], wide_roll(blocks[2 + m], 64, 1)
                    )
            else:
                for m in range(3):
                    out[owner, 8 * m : 8 * m + 8] = jnp.where(
                        section < 3, blocks[m], wide_roll(blocks[3], 32 * (3 - m), 1)
                    )

        def send(chip, target_core):
            remote(out.at[2 * chip + target_core], homes[kind].at[b], sems.at[n + 2], sems.at[n + 3], (chip, target_core))

        def step(k, carry):
            chip = chip_at(b, k % chips)
            pick(chip, 0)
            pick(chip, 1)

            @pl.when(k > 1)
            def _():
                before = chip_at(b, k - 1)
                send(before, 0)
                send(before, 1)

            return carry

        lax.fori_loop(1, chips + 1, step, 0)
        homes[kind][b] = out[2 * b + core]
        send(b, 1 - core)

    my_early = (c == 1) & has_early(b)
    pl.when(c == 1)(lambda: wait_for("late", number["late"], chips))
    pl.when(my_early)(lambda: serve("early"))
    pl.when(c == 0)(lambda: serve("late"))

    def finish(kind, mine, count):
        n = number[kind]
        for holds, held in ((True, mine), (False, jnp.logical_not(mine))):

            @pl.when(held)
            def _():
                wait_for(kind, n + 3, count - holds)
                if kind == "early" or holds:
                    wait_for(kind, n, count - holds)
                if holds:
                    wait_for(kind, n + 2, 2 * chips - 1)

    return finish, my_early, c


def kernel(chips, f_hbm, levels, plan, out_ref, *scratch):
    kinds = ("early", "late")
    take = iter(scratch)
    plan_all = next(take)
    lbm = [next(take) for _ in range(15)]
    sends, homes, outs = ({kind: next(take) for kind in kinds} for _ in range(3))
    wide, ordered, late_rows = next(take), next(take), next(take)
    plan_turned, inv_vec, inv_smem, local_sem, sems = take
    moving = migrate(chips, sends, late_rows, plan_all, homes, plan_turned, inv_vec, inv_smem, wide, ordered, outs, local_sem, sems)
    send_early = next(moving)
    drain, end_plan = lbm_steps(chips, f_hbm, levels, plan, sends, late_rows, plan_all, *lbm, send_early)
    try:
        moving.send(end_plan)
    except StopIteration as stop:
        finish, my_early, c = stop.value
    drain()
    for kind, mine, count in (("early", my_early, EARLY), ("late", c == 0, chips)):
        finish(kind, mine, count)
        for (q, ih), (where, place) in UNITS.items():
            if where != kind:
                continue
            lanes = pl.ds(128 * ih, 128)
            home = homes[kind]
            if kind == "early":
                first, second = lane_blocks([home[chip] for chip in place])
                out_ref[q, 0:16, lanes] = first
                out_ref[q, 16:32, lanes] = second
            else:
                columns = [divmod(4 * place + h, 3) for h in range(4)]
                for m in range(3):
                    out_ref[q, 8 * m : 8 * m + 8, lanes] = chosen(
                        [(home[chip, 8 * m : 8 * m + 8], i) for chip, i in columns]
                    )
                out_ref[q, 24:32, lanes] = chosen([(home[chip, 8 * i : 8 * i + 8], 3) for chip, i in columns])


def body(f_home, levels, plan):
    chips = lax.axis_size("blocks")
    f32, i32 = jnp.float32, jnp.int32
    dma = pltpu.SemaphoreType.DMA
    out = pl.pallas_call(
        lambda *refs: kernel(chips, *refs),
        out_shape=pltpu.VMEM((19, 32, 512), f32),
        in_specs=[pl.BlockSpec(memory_space=pltpu.HBM)] * 3,
        out_specs=pl.BlockSpec(memory_space=pltpu.VMEM),
        scratch_shapes=[
            pltpu.VMEM((2 * chips, 1, 128), i32),
            pltpu.SMEM((32,), i32),
            pltpu.SMEM((32,), i32),
            pltpu.VMEM((4, 19, 32, 128), f32),
            pltpu.VMEM((19, 4, 32, 128), f32),
            pltpu.VMEM((STEPS, 2, 19, 4, 6, 8, 128), f32),
            pltpu.VMEM((19, 4, 4, 8, 128), f32),
            pltpu.VMEM((STEPS, 2, 5, 4, 8, 128), f32),
            pltpu.VMEM((STEPS, 2, 5, 6, 8, 128), f32),
            pltpu.VMEM((3, 4, 8, 128), f32),
            dma((6,)),
            dma((STEPS, 16)),
            dma((STEPS, 16)),
            dma((4,)),
            dma((4,)),
            pltpu.SemaphoreType.REGULAR((3,)),
        ]
        + [pltpu.VMEM((64, size, 128), f32) for size in (16, 24)]
        + [pltpu.VMEM((64, size, 128), f32) for size in (16, 24)]
        + [pltpu.VMEM((2 * chips, size, 128), f32) for size in (16, 24)]
        + [pltpu.VMEM((64 * chips, 128), f32)] * 2
        + [pltpu.VMEM((48, 32, 128), f32)]
        + [
            pltpu.VMEM((128, 128), i32),
            pltpu.VMEM((128, 128), i32),
            pltpu.SMEM((128, 128), i32),
            dma,
            dma((8,)),
        ],
        compiler_params=pltpu.CompilerParams(
            collective_id=0, has_side_effects=True, vmem_limit_bytes=VMEM_LIMIT
        ),
        name="lattice_and_owners",
    )(f_home.transpose(1, 0, 2), levels, plan)
    return out.transpose(1, 0, 2)


def solution(mesh):
    spec = P(("blocks", "cross"))
    return jax.shard_map(
        body, mesh=mesh, in_specs=(spec, spec, spec), out_specs=spec, check_vma=False
    )
```

```python
import jax
import jax.numpy as jnp
from jax import lax
from jax.experimental import pallas as pl
from jax.experimental.pallas import tpu as pltpu
from jax.sharding import PartitionSpec as P

STEPS = 2
MESH = pl.DeviceIdType.MESH
VELOCITIES = (
    (0, 0, 0),
    (1, 0, 0),
    (-1, 0, 0),
    (0, 1, 0),
    (0, -1, 0),
    (0, 0, 1),
    (0, 0, -1),
    (1, 1, 0),
    (-1, -1, 0),
    (1, -1, 0),
    (-1, 1, 0),
    (1, 0, 1),
    (-1, 0, -1),
    (1, 0, -1),
    (-1, 0, 1),
    (0, 1, 1),
    (0, -1, -1),
    (0, 1, -1),
    (0, -1, 1),
)
WEIGHTS = (1.0 / 3.0,) + (1.0 / 18.0,) * 6 + (1.0 / 36.0,) * 12
PAIRS = tuple((q, q + 1) for q in range(1, 19, 2))
X_SPEEDS = ((1, 7, 9, 11, 13), (2, 8, 10, 12, 14))
Y_SPEEDS = ((3, 7, 10, 15, 17), (4, 8, 9, 16, 18))
TAU_COARSE = 0.55
TAU_FINE = 2.0 * TAU_COARSE - 0.5
RESCALE = TAU_FINE / (2.0 * TAU_COARSE)
INFLOW = 0.08


def row_units():
    early, late = [], []
    for q in range(19):
        for ih in range(4):
            ready = ((1, 2), (2,), (1,))[VELOCITIES[q][0]]
            (early if ih in ready else late).append((q, ih))
    chips = []
    for b in range(64):
        x, z, y = b // 16, b // 4 % 4, b % 4
        if (x + z) % 2 or y != (x + z) % 4:
            chips.append(b)
    units = {}
    for n, row in enumerate(early):
        units[row] = ("early", chips[2 * n : 2 * n + 2])
    for n, row in enumerate(late):
        units[row] = ("late", n)
    return units


UNITS = row_units()
EARLY = 56
VMEM_LIMIT = 56 * 1024 * 1024


def has_early(b):
    diagonal = mod(div(b, 16) + div(b, 4))
    return (lax.rem(diagonal, jnp.int32(2)) == 1) | (mod(b) != diagonal)


def inflow_value(speed):
    along = VELOCITIES[speed][0] * INFLOW
    return WEIGHTS[speed] * (1.0 + 3.0 * along + 4.5 * along * along - 1.5 * INFLOW * INFLOW)


def equilibrium(field):
    density = field[0]
    for q in range(1, 19):
        density = density + field[q]
    inverse = 1.0 / density
    velocity = []
    for axis in range(3):
        total = None
        for q in range(1, 19):
            sign = VELOCITIES[q][axis]
            if sign:
                if total is None:
                    total = field[q] if sign > 0 else -field[q]
                else:
                    total = total + field[q] if sign > 0 else total - field[q]
        velocity.append(total * inverse)
    ux, uy, uz = velocity
    base = 1.0 - 1.5 * (ux * ux + uy * uy + uz * uz)
    out = [None] * 19
    out[0] = WEIGHTS[0] * density * base
    for plus, minus in PAIRS:
        along = None
        for axis in range(3):
            sign = VELOCITIES[plus][axis]
            if sign:
                term = velocity[axis]
                if along is None:
                    along = term
                else:
                    along = along + term if sign > 0 else along - term
        even = base + 4.5 * along * along
        odd = 3.0 * along
        scale = WEIGHTS[plus] * density
        out[plus] = scale * (even + odd)
        out[minus] = scale * (even - odd)
    return out


def lattice_masks(shape):
    lane = lax.broadcasted_iota(jnp.int32, shape, len(shape) - 1)
    return lane, (lane // 8) % 8, lane % 8


def wide_roll(values, shift, axis):
    shift = shift % values.shape[axis]
    return values if shift == 0 else pltpu.roll(values, shift, axis)


def shifted(main, other, q):
    ex, ey, ez = VELOCITIES[q]
    n = main.shape[0]
    lane, j, k = lattice_masks((1, 8, 128))
    if ex > 0:
        main = jnp.where(lane[None] < 64, main, other)
    elif ex < 0:
        main = jnp.where(lane[None] >= 64, main, other)
    turn = 64 if ex else 0
    here = main[:, 1:5].reshape(4 * n, 8, 128)
    if ey > 0:
        there = main[:, 0:4].reshape(4 * n, 8, 128)
        here = jnp.where(j > 0, wide_roll(here, turn + 8, 2), wide_roll(there, turn - 56, 2))
        turn = 0
    elif ey < 0:
        there = main[:, 2:6].reshape(4 * n, 8, 128)
        here = jnp.where(j < 7, wide_roll(here, turn - 8, 2), wide_roll(there, turn + 56, 2))
        turn = 0
    if ez > 0:
        over = wide_roll(wide_roll(here, 1, 1), turn - 7, 2)
        here = jnp.where(k > 0, wide_roll(here, turn + 1, 2), over)
    elif ez < 0:
        over = wide_roll(wide_roll(here, 7, 1), turn + 7, 2)
        here = jnp.where(k < 7, wide_roll(here, turn - 1, 2), over)
    else:
        here = wide_roll(here, turn, 2)
    return here.reshape(n, 4, 8, 128)


def lane_blocks(parts):
    n = len(parts)
    section = lax.broadcasted_iota(jnp.int32, parts[0].shape, parts[0].ndim - 1) // (128 // n)
    out = []
    for h in range(n):
        total = parts[h]
        for m in range(n):
            if m != h:
                total = jnp.where(section == m, wide_roll(parts[m], 128 // n * (m - h), total.ndim - 1), total)
        out.append(total)
    return out


def chosen(parts):
    section = lax.broadcasted_iota(jnp.int32, (8, 128), 1) // 32
    total = None
    for h, (part, at) in enumerate(parts):
        part = wide_roll(part, 32 * (h - at), 1)
        total = part if total is None else jnp.where(section == h, part, total)
    return total


def shifted_inside(work, q, ih):
    ex, ey, ez = VELOCITIES[q]
    lane, j, k = lattice_masks((1, 8, 128))
    main = work[q, ih]
    inside = None

    def both_of(first, second):
        return second if first is None else first & second

    if ex:
        low = lane < 64
        if 0 <= ih - ex < 4:
            main = jnp.where(low if ex > 0 else ~low, main, work[q, ih - ex])
        else:
            inside = ~low if ex > 0 else low
    if ey:
        inside = both_of(inside, (j > 0) if ey > 0 else (j < 7))
    if ez:
        inside = both_of(inside, (k > 0) if ez > 0 else (k < 7))
    return wide_roll(main, (64 if ex else 0) + 8 * ey + ez, 2), inside


def lbm_steps(
    blocks, f_hbm, levels_hbm, plan_hbm, sends, late_rows, plan_all, levels, plan, raw, state, both, work, pack_x, halo_x, coef,
    load_sem, send_sem, recv_sem, round_send, round_recv, ready, send_early,
):
    b = lax.axis_index("blocks")
    c = lax.axis_index("cross")
    has_low, has_high = b > 0, b < blocks - 1
    low, high = jnp.maximum(b - 1, 0), jnp.minimum(b + 1, blocks - 1)

    loads = [
        pltpu.make_async_copy(
            f_hbm.at[:, :, pl.ds(128 * ih, 128)], raw.at[ih], load_sem.at[ih]
        )
        for ih in range(4)
    ]
    numbers = [
        pltpu.make_async_copy(levels_hbm, levels, load_sem.at[4]),
        pltpu.make_async_copy(plan_hbm, plan, load_sem.at[5]),
    ]
    for load in numbers + loads:
        load.start()

    barrier = pltpu.get_barrier_semaphore()

    def greet(device):
        pl.semaphore_signal(barrier, inc=1, device_id=device, device_id_type=MESH)

    greet((b, 1 - c))

    def line(axis):
        stride = (16, 4, 1)[axis]
        at = (b // stride) % 4
        return [b + stride * ((at + k) % 4 - at) for k in (1, 2, 3)]

    for axis in range(3):
        for chip in line(axis):
            greet((chip, c))

    @pl.when(has_low)
    def _():
        greet((low, c))
        greet((low, 1 - c))

    @pl.when(has_high)
    def _():
        greet((high, c))
        greet((high, 1 - c))

    for load in numbers:
        load.wait()
    sublane = lax.broadcasted_iota(jnp.int32, (8, 128), 0)
    for py in range(4):
        fine = jnp.zeros((8, 128), jnp.float32)
        for pz in range(8):
            fine = jnp.where(sublane == pz, levels[py * 8 + pz].astype(jnp.float32), fine)
        is_fine = fine > 0.5
        coef[0, py] = fine
        coef[1, py] = jnp.where(is_fine, (1.0 - 1.0 / TAU_FINE) / RESCALE, 1.0 - 1.0 / TAU_COARSE)
        coef[2, py] = jnp.where(is_fine, 1.0 - 1.0 / TAU_FINE, RESCALE * (1.0 - 1.0 / TAU_COARSE))

    for step in range(STEPS):
        for side in range(2):

            @pl.when(jnp.logical_not(has_low if side == 0 else has_high))
            def _():
                for n, q in enumerate(X_SPEEDS[side]):
                    halo_x[step, side, n] = jnp.full((6, 8, 128), inflow_value(q), jnp.float32)

    plan_row = jnp.zeros((1, 128), jnp.int32)
    plan_lane = lax.broadcasted_iota(jnp.int32, (1, 128), 1)
    for p in range(32):
        plan_row = jnp.where(plan_lane == p, plan[p], plan_row)
    plan_all[64 * c + b] = plan_row

    def plan_round(number):
        size = (1, 4, 16, 64)[number]
        part = plan_all.at[pl.ds(64 * c + (b // size) * size, size)]
        peers = [(b, 1 - c)] if number == 3 else [(chip, c) for chip in line(2 - number)]
        copies = [
            pltpu.make_async_remote_copy(
                src_ref=part,
                dst_ref=part,
                send_sem=round_send.at[number],
                recv_sem=round_recv.at[number],
                device_id=peer,
                device_id_type=MESH,
            )
            for peer in peers
        ]
        for copy in copies:
            copy.start()

    def end_round(number):
        moved = plan_all.at[pl.ds(0, (3, 12, 48, 64)[number])]
        pltpu.make_async_copy(moved, moved, round_recv.at[number]).wait()
        pltpu.make_async_copy(moved, moved, round_send.at[number]).wait()

    for load in loads:
        load.wait()

    lane = lax.broadcasted_iota(jnp.int32, (4, 8, 128), 2)
    pending = []

    def over_outer(body):
        def at(pos, carry):
            body(3 * (pos // 4), pos % 4)
            return carry

        lax.fori_loop(0, 8, at, 0)

    def over_inner(body):
        def at(pos, carry):
            body(1 + pos // 4, pos % 4)
            return carry

        lax.fori_loop(0, 8, at, 0)

    for step in range(STEPS):

        def relax_both(ih, py):
            rows_of_py = pl.ds(pl.multiple_of(py * 8, 8), 8)
            if step:
                field = [state[q, ih, rows_of_py, :] for q in range(19)]
            else:
                field = [raw[ih, q, rows_of_py, :] for q in range(19)]
            balance = equilibrium(field)
            for_coarse, for_fine = coef[1, py], coef[2, py]
            for q in range(19):
                away = field[q] - balance[q]
                both[step, 0, q, ih, py + 1] = balance[q] + for_coarse * away
                both[step, 1, q, ih, py + 1] = balance[q] + for_fine * away

        over_outer(relax_both)

        copies = []

        def add(src, dst, device, send_if, recv_if):
            index = len(copies)
            copy = pltpu.make_async_remote_copy(
                src_ref=src,
                dst_ref=dst,
                send_sem=send_sem.at[step, index],
                recv_sem=recv_sem.at[step, index],
                device_id=device,
                device_id_type=MESH,
            )
            copies.append((send_if, recv_if, copy))

        for side in range(2):
            edge = 3 if side == 0 else 0
            for n, q in enumerate(X_SPEEDS[side]):
                first = both[step, 0, q, edge, 1:5]
                second = pltpu.roll(both[step, 1, q, edge, 1:5], 64, 2)
                keep = lane >= 64 if side == 0 else lane < 64
                pack_x[step, side, n] = jnp.where(keep, first, second)
        if step == 0:
            pl.semaphore_wait(
                barrier, 10 + 2 * has_low.astype(jnp.int32) + 2 * has_high.astype(jnp.int32)
            )
            for chip in line(2):
                pl.semaphore_signal(ready.at[0], inc=1, device_id=(chip, c), device_id_type=MESH)
        for side in range(2):
            target = high if side == 0 else low
            send_if, recv_if = (has_high, has_low) if side == 0 else (has_low, has_high)
            add(
                pack_x.at[step, side],
                halo_x.at[step, side, :, pl.ds(1, 4)],
                (target, c),
                send_if,
                recv_if,
            )
            for n, q in enumerate(X_SPEEDS[side]):
                ey = VELOCITIES[q][1]
                if ey:
                    py, slot = (3, 0) if ey > 0 else (0, 5)
                    add(
                        pack_x.at[step, side, n, py],
                        halo_x.at[step, side, n, slot],
                        (target, 1 - c),
                        send_if,
                        recv_if,
                    )
        def start(chosen):
            for send_if, recv_if, copy in chosen:
                if send_if is None:
                    copy.start()
                else:
                    pl.when(send_if)(copy.start)

        def arrive(chosen):
            for send_if, recv_if, copy in chosen:
                if recv_if is None:
                    copy.wait_recv()
                else:
                    pl.when(recv_if)(copy.wait_recv)

        start(copies)
        along_x = len(copies)
        over_inner(relax_both)
        for side in range(2):
            py, slot = (4, 0) if side == 0 else (1, 5)
            for q in Y_SPEEDS[side]:
                add(
                    both.at[step, :, q, :, py],
                    both.at[step, :, q, :, slot],
                    (b, 1 - c),
                    None,
                    None,
                )
        start(copies[along_x:])
        if step == 0:
            plan_round(0)
        else:
            end_round(1)
            plan_round(2)
        fine = coef[0]

        def stream(q, first, last, halo):
            ex = VELOCITIES[q][0]
            result = []
            for kind in range(2):
                other = None
                if halo:
                    side = 0 if ex > 0 else 1
                    other = halo_x[step, side, X_SPEEDS[side].index(q)]
                    other = (pltpu.roll(other, 64, 2) if kind else other)[None]
                elif ex:
                    other = both[step, kind, q, first - ex : last - ex]
                result.append(shifted(both[step, kind, q, first:last], other, q))
            moved = jnp.where(fine[None] > 0.5, result[1], result[0])
            state[q, first:last] = moved.reshape(last - first, 32, 128)

        arrive(copies[along_x:])
        for q in range(19):
            ex = VELOCITIES[q][0]
            stream(q, 1 if ex > 0 else 0, 3 if ex < 0 else 4, False)

        def relax_again(ih, py):
            rows_of_py = pl.ds(pl.multiple_of(py * 8, 8), 8)
            field = [state[q, ih, rows_of_py, :] for q in range(19)]
            balance = equilibrium(field)
            for q in range(19):
                work[q, ih, py] = field[q] + (1.0 / TAU_FINE) * (balance[q] - field[q])

        def finish(q, ih):
            moved, inside = shifted_inside(work, q, ih)
            inside = fine > 0.5 if inside is None else inside & (fine > 0.5)
            result = jnp.where(inside, moved, state[q, ih].reshape(4, 8, 128)).reshape(32, 128)
            if step == STEPS - 1:
                kind, place = UNITS[q, ih]
                if kind == "late":
                    late_rows[place] = result
                else:
                    for chip, block in zip(place, lane_blocks([result[:16], result[16:]])):
                        sends[kind][chip] = block
            else:
                state[q, ih] = result

        if step == 0:
            pl.semaphore_wait(ready.at[0], 3)
            for chip in line(1):
                pl.semaphore_signal(ready.at[1], inc=1, device_id=(chip, c), device_id_type=MESH)
        over_inner(relax_again)
        last = step == STEPS - 1
        early = [row for row, unit in UNITS.items() if unit[0] == "early"]
        if last:
            for q, ih in early:
                finish(q, ih)
            pl.semaphore_wait(ready.at[2], 1)
            send_early()
        arrive(copies[:along_x])
        pending += copies
        if step == 0:
            end_round(0)
            plan_round(1)
            pl.semaphore_wait(ready.at[1], 3)
            pl.semaphore_signal(ready.at[2], inc=1, device_id=(b, 1 - c), device_id_type=MESH)
        else:
            end_round(2)
            plan_round(3)
        for side in range(2):
            for q in X_SPEEDS[side]:
                stream(q, 3 * side, 3 * side + 1, True)
        over_outer(relax_again)
        for q in range(19):
            for ih in range(4):
                if not (last and (q, ih) in early):
                    finish(q, ih)

    def drain():
        for send_if, recv_if, copy in pending:
            if send_if is None:
                copy.wait_send()
            else:
                pl.when(send_if)(copy.wait_send)

    return drain, lambda: end_round(3)


def mod(value):
    return lax.rem(value, jnp.int32(4))


def div(value, by):
    return lax.div(value, jnp.int32(by))


def chip_beside(b, dx, dz, dy):
    return 16 * mod(div(b, 16) + dx) + 4 * mod(div(b, 4) + dz) + mod(b + dy)


def chip_at(b, k):
    dz = k + div(k, 4)
    return chip_beside(b, k, dz, dz + div(k, 16))


OFFSETS = [
    (k % 4, (k + k // 4) % 4, (k + k // 4 + k // 16) % 4) for k in (*range(63, 0, -1), 0)
]


def migrate(chips, sends, late_rows, plan_all, homes, plan_turned, inv_vec, inv_smem, wide, ordered, outs, local_sem, sems):
    b = lax.axis_index("blocks")
    c = lax.axis_index("cross")
    source = 64 * c + b
    cores = {"early": 1, "late": 0}
    sizes = {"early": 16, "late": 24}

    def remote(src, dst, send, recv, device):
        pltpu.make_async_remote_copy(
            src_ref=src, dst_ref=dst, send_sem=send, recv_sem=recv, device_id=device, device_id_type=MESH
        ).start()

    def wait_for(kind, sem, count):
        part = wide.at[pl.ds(0, sizes[kind] * count)]
        pltpu.make_async_copy(part, part, sems.at[sem]).wait()

    number = {"early": 0, "late": 4}

    def spread(kind, offset):
        chip = chip_beside(b, *offset)

        def send():
            n = number[kind]
            land = wide.at[pl.ds(pl.multiple_of(source * 32, 32), sizes[kind])]
            remote(sends[kind].at[chip], land, sems.at[n], sems.at[n + 1], (chip, cores[kind]))

        if kind == "early":
            wanted = has_early(chip)
            pl.when(wanted if any(offset) else wanted & (c != cores[kind]))(send)
        elif any(offset):
            send()
        else:
            pl.when(c != cores[kind])(send)

    def send_early():
        for offset in OFFSETS:
            spread("early", offset)

    end_plan = yield send_early

    for chip in range(64):
        columns = [divmod(3 * chip + i, 4) for i in range(3)]
        for m in range(3):
            parts = [(late_rows[n, 8 * m : 8 * m + 8], h) for n, h in columns]
            n, h = columns[m]
            sends["late"][chip, 8 * m : 8 * m + 8] = chosen(parts + [(late_rows[n, 24:32], h)])

    for offset in OFFSETS:
        spread("late", offset)
    end_plan()

    plans = plan_all[:, 0, :]
    plan_turned[...] = plans.T
    sub = lax.broadcasted_iota(jnp.int32, (128, 128), 0)
    lane = lax.broadcasted_iota(jnp.int32, (128, 128), 1)

    def place(p, carry):
        plans, total = carry
        owner = plan_turned[pl.ds(p, 1), :] // 32
        hot = jnp.where(owner == sub, 1.0, 0.0)
        slot = plans[:, 0:1] % 32
        value = jnp.where(slot == lane, sub, jnp.where(slot + 32 == lane, p, 0))
        total = total + jnp.dot(
            hot.astype(jnp.bfloat16),
            value.astype(jnp.float32).astype(jnp.bfloat16),
            preferred_element_type=jnp.float32,
        )
        return pltpu.roll(plans, 127, 1), total

    _, total = lax.fori_loop(0, 32, place, (plans, jnp.zeros((128, 128), jnp.float32)), unroll=4)
    total = total.astype(jnp.int32)
    inv_vec[...] = jnp.clip(total * 32 + pltpu.roll(total, 96, 1), 0, 64 * chips - 1)
    move = pltpu.make_async_copy(inv_vec, inv_smem, local_sem)
    move.start()
    move.wait()

    def serve(kind):
        out, size, n = outs[kind], sizes[kind], number[kind]
        core = cores[kind]
        wide[pl.ds(pl.multiple_of(source * 32, 32), size), :] = sends[kind][b]
        wait_for(kind, n + 1, 2 * chips - 1)
        section = lax.broadcasted_iota(jnp.int32, (8, 128), 1) // 32

        def widen(s, carry):
            at = lambda m: pl.ds(pl.multiple_of(s * 32 + 8 * m, 8), 8)
            if kind == "early":
                for m in range(2):
                    wide[at(2 + m), :] = wide_roll(wide[at(m), :], 64, 1)
            else:
                wide[at(3), :] = chosen([(wide[at(m), :], 3) for m in range(3)])
            return carry

        lax.fori_loop(0, 2 * chips, widen, 0, unroll=8)

        def pick(chip, target_core):
            owner = 2 * chip + target_core
            for u in range(32):
                index = inv_smem[owner, u]
                ordered[pl.ds(owner * 32 + u, 1), :] = wide[pl.ds(index, 1), :]
            blocks = [ordered[pl.ds(pl.multiple_of(owner * 32 + 8 * m, 8), 8), :] for m in range(4)]
            if kind == "early":
                for m in range(2):
                    out[owner, 8 * m : 8 * m + 8] = jnp.where(
                        section < 2, blocks[m], wide_roll(blocks[2 + m], 64, 1)
                    )
            else:
                for m in range(3):
                    out[owner, 8 * m : 8 * m + 8] = jnp.where(
                        section < 3, blocks[m], wide_roll(blocks[3], 32 * (3 - m), 1)
                    )

        def send(chip, target_core):
            remote(out.at[2 * chip + target_core], homes[kind].at[b], sems.at[n + 2], sems.at[n + 3], (chip, target_core))

        def step(k, before):
            chip = chip_at(b, chips - k)
            pick(chip, 0)
            pick(chip, 1)

            @pl.when(k > 1)
            def _():
                send(before, 0)
                send(before, 1)

            return chip

        lax.fori_loop(1, chips + 1, step, b)
        homes[kind][b] = out[2 * b + core]
        send(b, 1 - core)

    my_early = (c == 1) & has_early(b)
    pl.when(c == 1)(lambda: wait_for("late", number["late"], chips))
    pl.when(my_early)(lambda: serve("early"))
    pl.when(c == 0)(lambda: serve("late"))

    def finish(kind, mine, count):
        n = number[kind]
        for holds, held in ((True, mine), (False, jnp.logical_not(mine))):

            @pl.when(held)
            def _():
                wait_for(kind, n + 3, count - holds)
                if kind == "early" or holds:
                    wait_for(kind, n, count - holds)
                if holds:
                    wait_for(kind, n + 2, 2 * chips - 1)

    return finish, my_early, c


def kernel(chips, f_hbm, levels, plan, out_ref, *scratch):
    kinds = ("early", "late")
    take = iter(scratch)
    plan_all = next(take)
    lbm = [next(take) for _ in range(15)]
    sends, homes, outs = ({kind: next(take) for kind in kinds} for _ in range(3))
    wide, ordered, late_rows = next(take), next(take), next(take)
    plan_turned, inv_vec, inv_smem, local_sem, sems = take
    moving = migrate(chips, sends, late_rows, plan_all, homes, plan_turned, inv_vec, inv_smem, wide, ordered, outs, local_sem, sems)
    send_early = next(moving)
    drain, end_plan = lbm_steps(chips, f_hbm, levels, plan, sends, late_rows, plan_all, *lbm, send_early)
    try:
        moving.send(end_plan)
    except StopIteration as stop:
        finish, my_early, c = stop.value
    drain()
    for kind, mine, count in (("early", my_early, EARLY), ("late", c == 0, chips)):
        finish(kind, mine, count)
        for (q, ih), (where, place) in UNITS.items():
            if where != kind:
                continue
            lanes = pl.ds(128 * ih, 128)
            home = homes[kind]
            if kind == "early":
                first, second = lane_blocks([home[chip] for chip in place])
                out_ref[q, 0:16, lanes] = first
                out_ref[q, 16:32, lanes] = second
            else:
                columns = [divmod(4 * place + h, 3) for h in range(4)]
                for m in range(3):
                    out_ref[q, 8 * m : 8 * m + 8, lanes] = chosen(
                        [(home[chip, 8 * m : 8 * m + 8], i) for chip, i in columns]
                    )
                out_ref[q, 24:32, lanes] = chosen([(home[chip, 8 * i : 8 * i + 8], 3) for chip, i in columns])


def body(f_home, levels, plan):
    chips = lax.axis_size("blocks")
    f32, i32 = jnp.float32, jnp.int32
    dma = pltpu.SemaphoreType.DMA
    out = pl.pallas_call(
        lambda *refs: kernel(chips, *refs),
        out_shape=pltpu.VMEM((19, 32, 512), f32),
        in_specs=[pl.BlockSpec(memory_space=pltpu.HBM)] * 3,
        out_specs=pl.BlockSpec(memory_space=pltpu.VMEM),
        scratch_shapes=[
            pltpu.VMEM((2 * chips, 1, 128), i32),
            pltpu.SMEM((32,), i32),
            pltpu.SMEM((32,), i32),
            pltpu.VMEM((4, 19, 32, 128), f32),
            pltpu.VMEM((19, 4, 32, 128), f32),
            pltpu.VMEM((STEPS, 2, 19, 4, 6, 8, 128), f32),
            pltpu.VMEM((19, 4, 4, 8, 128), f32),
            pltpu.VMEM((STEPS, 2, 5, 4, 8, 128), f32),
            pltpu.VMEM((STEPS, 2, 5, 6, 8, 128), f32),
            pltpu.VMEM((3, 4, 8, 128), f32),
            dma((6,)),
            dma((STEPS, 16)),
            dma((STEPS, 16)),
            dma((4,)),
            dma((4,)),
            pltpu.SemaphoreType.REGULAR((3,)),
        ]
        + [pltpu.VMEM((64, size, 128), f32) for size in (16, 24)]
        + [pltpu.VMEM((64, size, 128), f32) for size in (16, 24)]
        + [pltpu.VMEM((2 * chips, size, 128), f32) for size in (16, 24)]
        + [pltpu.VMEM((64 * chips, 128), f32)] * 2
        + [pltpu.VMEM((48, 32, 128), f32)]
        + [
            pltpu.VMEM((128, 128), i32),
            pltpu.VMEM((128, 128), i32),
            pltpu.SMEM((128, 128), i32),
            dma,
            dma((8,)),
        ],
        compiler_params=pltpu.CompilerParams(
            collective_id=0, has_side_effects=True, vmem_limit_bytes=VMEM_LIMIT
        ),
        name="lattice_and_owners",
    )(f_home.transpose(1, 0, 2), levels, plan)
    return out.transpose(1, 0, 2)


def solution(mesh):
    spec = P(("blocks", "cross"))
    return jax.shard_map(
        body, mesh=mesh, in_specs=(spec, spec, spec), out_specs=spec, check_vma=False
    )
```

```python
import jax
import jax.numpy as jnp
from jax import lax
from jax.experimental import pallas as pl
from jax.experimental.pallas import tpu as pltpu
from jax.sharding import PartitionSpec as P

STEPS = 2
MESH = pl.DeviceIdType.MESH
VELOCITIES = (
    (0, 0, 0),
    (1, 0, 0),
    (-1, 0, 0),
    (0, 1, 0),
    (0, -1, 0),
    (0, 0, 1),
    (0, 0, -1),
    (1, 1, 0),
    (-1, -1, 0),
    (1, -1, 0),
    (-1, 1, 0),
    (1, 0, 1),
    (-1, 0, -1),
    (1, 0, -1),
    (-1, 0, 1),
    (0, 1, 1),
    (0, -1, -1),
    (0, 1, -1),
    (0, -1, 1),
)
WEIGHTS = (1.0 / 3.0,) + (1.0 / 18.0,) * 6 + (1.0 / 36.0,) * 12
PAIRS = tuple((q, q + 1) for q in range(1, 19, 2))
X_SPEEDS = ((1, 7, 9, 11, 13), (2, 8, 10, 12, 14))
Y_SPEEDS = ((3, 7, 10, 15, 17), (4, 8, 9, 16, 18))
TAU_COARSE = 0.55
TAU_FINE = 2.0 * TAU_COARSE - 0.5
RESCALE = TAU_FINE / (2.0 * TAU_COARSE)
INFLOW = 0.08


def row_units():
    early, late = [], []
    for q in range(19):
        for ih in range(4):
            ready = ((1, 2), (2,), (1,))[VELOCITIES[q][0]]
            (early if ih in ready else late).append((q, ih))
    chips = []
    for b in range(64):
        x, z, y = b // 16, b // 4 % 4, b % 4
        if (x + z) % 2 or y != (x + z) % 4:
            chips.append(b)
    units = {}
    for n, row in enumerate(early):
        units[row] = ("early", chips[2 * n : 2 * n + 2])
    for n, row in enumerate(late):
        units[row] = ("late", n)
    return units


UNITS = row_units()
EARLY = 56
VMEM_LIMIT = 56 * 1024 * 1024


def has_early(b):
    diagonal = mod(div(b, 16) + div(b, 4))
    return (lax.rem(diagonal, jnp.int32(2)) == 1) | (mod(b) != diagonal)


def inflow_value(speed):
    along = VELOCITIES[speed][0] * INFLOW
    return WEIGHTS[speed] * (1.0 + 3.0 * along + 4.5 * along * along - 1.5 * INFLOW * INFLOW)


def equilibrium(field):
    density = field[0]
    for q in range(1, 19):
        density = density + field[q]
    inverse = 1.0 / density
    velocity = []
    for axis in range(3):
        total = None
        for q in range(1, 19):
            sign = VELOCITIES[q][axis]
            if sign:
                if total is None:
                    total = field[q] if sign > 0 else -field[q]
                else:
                    total = total + field[q] if sign > 0 else total - field[q]
        velocity.append(total * inverse)
    ux, uy, uz = velocity
    base = 1.0 - 1.5 * (ux * ux + uy * uy + uz * uz)
    out = [None] * 19
    out[0] = WEIGHTS[0] * density * base
    for plus, minus in PAIRS:
        along = None
        for axis in range(3):
            sign = VELOCITIES[plus][axis]
            if sign:
                term = velocity[axis]
                if along is None:
                    along = term
                else:
                    along = along + term if sign > 0 else along - term
        even = base + 4.5 * along * along
        odd = 3.0 * along
        scale = WEIGHTS[plus] * density
        out[plus] = scale * (even + odd)
        out[minus] = scale * (even - odd)
    return out


def lattice_masks(shape):
    lane = lax.broadcasted_iota(jnp.int32, shape, len(shape) - 1)
    return lane, (lane // 8) % 8, lane % 8


def wide_roll(values, shift, axis):
    shift = shift % values.shape[axis]
    return values if shift == 0 else pltpu.roll(values, shift, axis)


def shifted(main, other, q):
    ex, ey, ez = VELOCITIES[q]
    n = main.shape[0]
    lane, j, k = lattice_masks((1, 8, 128))
    if ex > 0:
        main = jnp.where(lane[None] < 64, main, other)
    elif ex < 0:
        main = jnp.where(lane[None] >= 64, main, other)
    turn = 64 if ex else 0
    here = main[:, 1:5].reshape(4 * n, 8, 128)
    if ey > 0:
        there = main[:, 0:4].reshape(4 * n, 8, 128)
        here = jnp.where(j > 0, wide_roll(here, turn + 8, 2), wide_roll(there, turn - 56, 2))
        turn = 0
    elif ey < 0:
        there = main[:, 2:6].reshape(4 * n, 8, 128)
        here = jnp.where(j < 7, wide_roll(here, turn - 8, 2), wide_roll(there, turn + 56, 2))
        turn = 0
    if ez > 0:
        over = wide_roll(wide_roll(here, 1, 1), turn - 7, 2)
        here = jnp.where(k > 0, wide_roll(here, turn + 1, 2), over)
    elif ez < 0:
        over = wide_roll(wide_roll(here, 7, 1), turn + 7, 2)
        here = jnp.where(k < 7, wide_roll(here, turn - 1, 2), over)
    else:
        here = wide_roll(here, turn, 2)
    return here.reshape(n, 4, 8, 128)


def lane_blocks(parts):
    n = len(parts)
    section = lax.broadcasted_iota(jnp.int32, parts[0].shape, parts[0].ndim - 1) // (128 // n)
    out = []
    for h in range(n):
        total = parts[h]
        for m in range(n):
            if m != h:
                total = jnp.where(section == m, wide_roll(parts[m], 128 // n * (m - h), total.ndim - 1), total)
        out.append(total)
    return out


def chosen(parts):
    section = lax.broadcasted_iota(jnp.int32, (8, 128), 1) // 32
    total = None
    for h, (part, at) in enumerate(parts):
        part = wide_roll(part, 32 * (h - at), 1)
        total = part if total is None else jnp.where(section == h, part, total)
    return total


def shifted_inside(work, q, ih):
    ex, ey, ez = VELOCITIES[q]
    lane, j, k = lattice_masks((1, 8, 128))
    main = work[q, ih]
    inside = None

    def both_of(first, second):
        return second if first is None else first & second

    if ex:
        low = lane < 64
        if 0 <= ih - ex < 4:
            main = jnp.where(low if ex > 0 else ~low, main, work[q, ih - ex])
        else:
            inside = ~low if ex > 0 else low
    if ey:
        inside = both_of(inside, (j > 0) if ey > 0 else (j < 7))
    if ez:
        inside = both_of(inside, (k > 0) if ez > 0 else (k < 7))
    return wide_roll(main, (64 if ex else 0) + 8 * ey + ez, 2), inside


def lbm_steps(
    blocks, f_hbm, levels_hbm, plan_hbm, sends, late_rows, plan_all, levels, plan, raw, state, both, work, pack_x, halo_x, coef,
    load_sem, send_sem, recv_sem, round_send, round_recv, ready, send_early,
):
    b = lax.axis_index("blocks")
    c = lax.axis_index("cross")
    has_low, has_high = b > 0, b < blocks - 1
    low, high = jnp.maximum(b - 1, 0), jnp.minimum(b + 1, blocks - 1)

    loads = [
        pltpu.make_async_copy(
            f_hbm.at[:, :, pl.ds(128 * ih, 128)], raw.at[ih], load_sem.at[ih]
        )
        for ih in range(4)
    ]
    numbers = [
        pltpu.make_async_copy(levels_hbm, levels, load_sem.at[4]),
        pltpu.make_async_copy(plan_hbm, plan, load_sem.at[5]),
    ]
    for load in numbers + loads:
        load.start()

    barrier = pltpu.get_barrier_semaphore()

    def greet(device):
        pl.semaphore_signal(barrier, inc=1, device_id=device, device_id_type=MESH)

    greet((b, 1 - c))

    def line(axis):
        stride = (16, 4, 1)[axis]
        at = (b // stride) % 4
        return [b + stride * ((at + k) % 4 - at) for k in (1, 2, 3)]

    for axis in range(3):
        for chip in line(axis):
            greet((chip, c))

    @pl.when(has_low)
    def _():
        greet((low, c))
        greet((low, 1 - c))

    @pl.when(has_high)
    def _():
        greet((high, c))
        greet((high, 1 - c))

    for load in numbers:
        load.wait()
    sublane = lax.broadcasted_iota(jnp.int32, (8, 128), 0)
    for py in range(4):
        fine = jnp.zeros((8, 128), jnp.float32)
        for pz in range(8):
            fine = jnp.where(sublane == pz, levels[py * 8 + pz].astype(jnp.float32), fine)
        is_fine = fine > 0.5
        coef[0, py] = fine
        coef[1, py] = jnp.where(is_fine, (1.0 - 1.0 / TAU_FINE) / RESCALE, 1.0 - 1.0 / TAU_COARSE)
        coef[2, py] = jnp.where(is_fine, 1.0 - 1.0 / TAU_FINE, RESCALE * (1.0 - 1.0 / TAU_COARSE))

    for step in range(STEPS):
        for side in range(2):

            @pl.when(jnp.logical_not(has_low if side == 0 else has_high))
            def _():
                for n, q in enumerate(X_SPEEDS[side]):
                    halo_x[step, side, n] = jnp.full((6, 8, 128), inflow_value(q), jnp.float32)

    plan_row = jnp.zeros((1, 128), jnp.int32)
    plan_lane = lax.broadcasted_iota(jnp.int32, (1, 128), 1)
    for p in range(32):
        plan_row = jnp.where(plan_lane == p, plan[p], plan_row)
    plan_all[64 * c + b] = plan_row

    def plan_round(number):
        size = (1, 4, 16, 64)[number]
        part = plan_all.at[pl.ds(64 * c + (b // size) * size, size)]
        peers = [(b, 1 - c)] if number == 3 else [(chip, c) for chip in line(2 - number)]
        copies = [
            pltpu.make_async_remote_copy(
                src_ref=part,
                dst_ref=part,
                send_sem=round_send.at[number],
                recv_sem=round_recv.at[number],
                device_id=peer,
                device_id_type=MESH,
            )
            for peer in peers
        ]
        for copy in copies:
            copy.start()

    def end_round(number):
        moved = plan_all.at[pl.ds(0, (3, 12, 48, 64)[number])]
        pltpu.make_async_copy(moved, moved, round_recv.at[number]).wait()
        pltpu.make_async_copy(moved, moved, round_send.at[number]).wait()

    for load in loads:
        load.wait()

    lane = lax.broadcasted_iota(jnp.int32, (4, 8, 128), 2)
    pending = []

    def over_outer(body):
        def at(pos, carry):
            body(3 * (pos // 4), pos % 4)
            return carry

        lax.fori_loop(0, 8, at, 0)

    def over_inner(body):
        def at(pos, carry):
            body(1 + pos // 4, pos % 4)
            return carry

        lax.fori_loop(0, 8, at, 0)

    for step in range(STEPS):

        def relax_both(ih, py):
            rows_of_py = pl.ds(pl.multiple_of(py * 8, 8), 8)
            if step:
                field = [state[q, ih, rows_of_py, :] for q in range(19)]
            else:
                field = [raw[ih, q, rows_of_py, :] for q in range(19)]
            balance = equilibrium(field)
            for_coarse, for_fine = coef[1, py], coef[2, py]
            for q in range(19):
                away = field[q] - balance[q]
                both[step, 0, q, ih, py + 1] = balance[q] + for_coarse * away
                both[step, 1, q, ih, py + 1] = balance[q] + for_fine * away

        over_outer(relax_both)

        copies = []

        def add(src, dst, device, send_if, recv_if):
            index = len(copies)
            copy = pltpu.make_async_remote_copy(
                src_ref=src,
                dst_ref=dst,
                send_sem=send_sem.at[step, index],
                recv_sem=recv_sem.at[step, index],
                device_id=device,
                device_id_type=MESH,
            )
            copies.append((send_if, recv_if, copy))

        for side in range(2):
            edge = 3 if side == 0 else 0
            for n, q in enumerate(X_SPEEDS[side]):
                first = both[step, 0, q, edge, 1:5]
                second = pltpu.roll(both[step, 1, q, edge, 1:5], 64, 2)
                keep = lane >= 64 if side == 0 else lane < 64
                pack_x[step, side, n] = jnp.where(keep, first, second)
        if step == 0:
            pl.semaphore_wait(
                barrier, 10 + 2 * has_low.astype(jnp.int32) + 2 * has_high.astype(jnp.int32)
            )
            for chip in line(2):
                pl.semaphore_signal(ready.at[0], inc=1, device_id=(chip, c), device_id_type=MESH)
        for side in range(2):
            target = high if side == 0 else low
            send_if, recv_if = (has_high, has_low) if side == 0 else (has_low, has_high)
            add(
                pack_x.at[step, side],
                halo_x.at[step, side, :, pl.ds(1, 4)],
                (target, c),
                send_if,
                recv_if,
            )
            for n, q in enumerate(X_SPEEDS[side]):
                ey = VELOCITIES[q][1]
                if ey:
                    py, slot = (3, 0) if ey > 0 else (0, 5)
                    add(
                        pack_x.at[step, side, n, py],
                        halo_x.at[step, side, n, slot],
                        (target, 1 - c),
                        send_if,
                        recv_if,
                    )
        def start(chosen):
            for send_if, recv_if, copy in chosen:
                if send_if is None:
                    copy.start()
                else:
                    pl.when(send_if)(copy.start)

        def arrive(chosen):
            for send_if, recv_if, copy in chosen:
                if recv_if is None:
                    copy.wait_recv()
                else:
                    pl.when(recv_if)(copy.wait_recv)

        start(copies)
        along_x = len(copies)
        over_inner(relax_both)
        for side in range(2):
            py, slot = (4, 0) if side == 0 else (1, 5)
            for q in Y_SPEEDS[side]:
                add(
                    both.at[step, :, q, :, py],
                    both.at[step, :, q, :, slot],
                    (b, 1 - c),
                    None,
                    None,
                )
        start(copies[along_x:])
        if step == 0:
            plan_round(0)
        else:
            end_round(1)
            plan_round(2)
        fine = coef[0]

        def stream(q, first, last, halo):
            ex = VELOCITIES[q][0]
            result = []
            for kind in range(2):
                other = None
                if halo:
                    side = 0 if ex > 0 else 1
                    other = halo_x[step, side, X_SPEEDS[side].index(q)]
                    other = (pltpu.roll(other, 64, 2) if kind else other)[None]
                elif ex:
                    other = both[step, kind, q, first - ex : last - ex]
                result.append(shifted(both[step, kind, q, first:last], other, q))
            moved = jnp.where(fine[None] > 0.5, result[1], result[0])
            state[q, first:last] = moved.reshape(last - first, 32, 128)

        arrive(copies[along_x:])
        for q in range(19):
            ex = VELOCITIES[q][0]
            stream(q, 1 if ex > 0 else 0, 3 if ex < 0 else 4, False)

        def relax_again(ih, py):
            rows_of_py = pl.ds(pl.multiple_of(py * 8, 8), 8)
            field = [state[q, ih, rows_of_py, :] for q in range(19)]
            balance = equilibrium(field)
            for q in range(19):
                work[q, ih, py] = field[q] + (1.0 / TAU_FINE) * (balance[q] - field[q])

        def finish(q, ih):
            moved, inside = shifted_inside(work, q, ih)
            inside = fine > 0.5 if inside is None else inside & (fine > 0.5)
            result = jnp.where(inside, moved, state[q, ih].reshape(4, 8, 128)).reshape(32, 128)
            if step == STEPS - 1:
                kind, place = UNITS[q, ih]
                if kind == "late":
                    late_rows[place] = result
                else:
                    for chip, block in zip(place, lane_blocks([result[:16], result[16:]])):
                        sends[kind][chip] = block
            else:
                state[q, ih] = result

        if step == 0:
            pl.semaphore_wait(ready.at[0], 3)
            for chip in line(1):
                pl.semaphore_signal(ready.at[1], inc=1, device_id=(chip, c), device_id_type=MESH)
        over_inner(relax_again)
        last = step == STEPS - 1
        early = [row for row, unit in UNITS.items() if unit[0] == "early"]
        if last:
            for q, ih in early:
                finish(q, ih)
            pl.semaphore_wait(ready.at[2], 1)
            send_early()
        arrive(copies[:along_x])
        pending += copies
        if step == 0:
            end_round(0)
            plan_round(1)
            pl.semaphore_wait(ready.at[1], 3)
            pl.semaphore_signal(ready.at[2], inc=1, device_id=(b, 1 - c), device_id_type=MESH)
        else:
            end_round(2)
            plan_round(3)
        for side in range(2):
            for q in X_SPEEDS[side]:
                stream(q, 3 * side, 3 * side + 1, True)
        over_outer(relax_again)
        for q in range(19):
            for ih in range(4):
                if not (last and (q, ih) in early):
                    finish(q, ih)

    def drain():
        for send_if, recv_if, copy in pending:
            if send_if is None:
                copy.wait_send()
            else:
                pl.when(send_if)(copy.wait_send)

    return drain, lambda: end_round(3)


def mod(value):
    return lax.rem(value, jnp.int32(4))


def div(value, by):
    return lax.div(value, jnp.int32(by))


def chip_beside(b, dx, dz, dy):
    return 16 * mod(div(b, 16) + dx) + 4 * mod(div(b, 4) + dz) + mod(b + dy)


def chip_at(b, k):
    dz = k + div(k, 4)
    return chip_beside(b, k, dz, dz + div(k, 16))


OFFSETS = [
    (k % 4, (k + k // 4) % 4, (k + k // 4 + k // 16) % 4) for k in (*range(63, 0, -1), 0)
]


def migrate(chips, sends, late_rows, plan_all, homes, plan_turned, inv_vec, inv_smem, wide, ordered, outs, local_sem, sems):
    b = lax.axis_index("blocks")
    c = lax.axis_index("cross")
    source = 64 * c + b
    cores = {"early": 1, "late": 0}
    sizes = {"early": 16, "late": 24}

    def remote(src, dst, send, recv, device):
        pltpu.make_async_remote_copy(
            src_ref=src, dst_ref=dst, send_sem=send, recv_sem=recv, device_id=device, device_id_type=MESH
        ).start()

    def wait_for(kind, sem, count):
        part = wide.at[pl.ds(0, sizes[kind] * count)]
        pltpu.make_async_copy(part, part, sems.at[sem]).wait()

    number = {"early": 0, "late": 4}

    def spread(kind, offset):
        chip = chip_beside(b, *offset)

        def send():
            n = number[kind]
            land = wide.at[pl.ds(pl.multiple_of(source * 32, 32), sizes[kind])]
            remote(sends[kind].at[chip], land, sems.at[n], sems.at[n + 1], (chip, cores[kind]))

        if kind == "early":
            wanted = has_early(chip)
            pl.when(wanted if any(offset) else wanted & (c != cores[kind]))(send)
        elif any(offset):
            send()
        else:
            pl.when(c != cores[kind])(send)

    def send_early():
        for offset in OFFSETS:
            spread("early", offset)

    end_plan = yield send_early

    for chip in range(64):
        columns = [divmod(3 * chip + i, 4) for i in range(3)]
        for m in range(3):
            parts = [(late_rows[n, 8 * m : 8 * m + 8], h) for n, h in columns]
            n, h = columns[m]
            sends["late"][chip, 8 * m : 8 * m + 8] = chosen(parts + [(late_rows[n, 24:32], h)])

    for offset in OFFSETS:
        spread("late", offset)
    end_plan()

    plans = plan_all[:, 0, :]
    plan_turned[...] = plans.T
    sub = lax.broadcasted_iota(jnp.int32, (128, 128), 0)
    lane = lax.broadcasted_iota(jnp.int32, (128, 128), 1)

    def place(p, carry):
        plans, total = carry
        owner = plan_turned[pl.ds(p, 1), :] // 32
        hot = jnp.where(owner == sub, 1.0, 0.0)
        slot = plans[:, 0:1] % 32
        value = jnp.where(slot == lane, sub, jnp.where(slot + 32 == lane, p, 0))
        total = total + jnp.dot(
            hot.astype(jnp.bfloat16),
            value.astype(jnp.float32).astype(jnp.bfloat16),
            preferred_element_type=jnp.float32,
        )
        return pltpu.roll(plans, 127, 1), total

    _, total = lax.fori_loop(0, 32, place, (plans, jnp.zeros((128, 128), jnp.float32)), unroll=4)
    total = total.astype(jnp.int32)
    inv_vec[...] = jnp.clip(total * 32 + pltpu.roll(total, 96, 1), 0, 64 * chips - 1)
    move = pltpu.make_async_copy(inv_vec, inv_smem, local_sem)
    move.start()
    move.wait()

    def serve(kind):
        out, size, n = outs[kind], sizes[kind], number[kind]
        core = cores[kind]
        wide[pl.ds(pl.multiple_of(source * 32, 32), size), :] = sends[kind][b]
        wait_for(kind, n + 1, 2 * chips - 1)
        section = lax.broadcasted_iota(jnp.int32, (8, 128), 1) // 32

        def widen(s, carry):
            at = lambda m: pl.ds(pl.multiple_of(s * 32 + 8 * m, 8), 8)
            if kind == "early":
                for m in range(2):
                    wide[at(2 + m), :] = wide_roll(wide[at(m), :], 64, 1)
            else:
                wide[at(3), :] = chosen([(wide[at(m), :], 3) for m in range(3)])
            return carry

        lax.fori_loop(0, 2 * chips, widen, 0, unroll=32)

        def pick(chip, target_core):
            owner = 2 * chip + target_core
            for u in range(32):
                index = inv_smem[owner, u]
                ordered[pl.ds(owner * 32 + u, 1), :] = wide[pl.ds(index, 1), :]
            blocks = [ordered[pl.ds(pl.multiple_of(owner * 32 + 8 * m, 8), 8), :] for m in range(4)]
            if kind == "early":
                for m in range(2):
                    out[owner, 8 * m : 8 * m + 8] = jnp.where(
                        section < 2, blocks[m], wide_roll(blocks[2 + m], 64, 1)
                    )
            else:
                for m in range(3):
                    out[owner, 8 * m : 8 * m + 8] = jnp.where(
                        section < 3, blocks[m], wide_roll(blocks[3], 32 * (3 - m), 1)
                    )

        def send(chip, target_core):
            remote(out.at[2 * chip + target_core], homes[kind].at[b], sems.at[n + 2], sems.at[n + 3], (chip, target_core))

        def step(k, before):
            chip = chip_at(b, chips - k)
            pick(chip, 0)
            pick(chip, 1)

            @pl.when(k > 1)
            def _():
                send(before, 0)
                send(before, 1)

            return chip

        lax.fori_loop(1, chips + 1, step, b)
        homes[kind][b] = out[2 * b + core]
        send(b, 1 - core)

    my_early = (c == 1) & has_early(b)
    pl.when(c == 1)(lambda: wait_for("late", number["late"], chips))
    pl.when(my_early)(lambda: serve("early"))
    pl.when(c == 0)(lambda: serve("late"))

    def finish(kind, mine, count):
        n = number[kind]
        for holds, held in ((True, mine), (False, jnp.logical_not(mine))):

            @pl.when(held)
            def _():
                wait_for(kind, n + 3, count - holds)
                if kind == "early" or holds:
                    wait_for(kind, n, count - holds)
                if holds:
                    wait_for(kind, n + 2, 2 * chips - 1)

    return finish, my_early, c


def kernel(chips, f_hbm, levels, plan, out_ref, *scratch):
    kinds = ("early", "late")
    take = iter(scratch)
    plan_all = next(take)
    lbm = [next(take) for _ in range(15)]
    sends, homes, outs = ({kind: next(take) for kind in kinds} for _ in range(3))
    wide, ordered, late_rows = next(take), next(take), next(take)
    plan_turned, inv_vec, inv_smem, local_sem, sems = take
    moving = migrate(chips, sends, late_rows, plan_all, homes, plan_turned, inv_vec, inv_smem, wide, ordered, outs, local_sem, sems)
    send_early = next(moving)
    drain, end_plan = lbm_steps(chips, f_hbm, levels, plan, sends, late_rows, plan_all, *lbm, send_early)
    try:
        moving.send(end_plan)
    except StopIteration as stop:
        finish, my_early, c = stop.value
    drain()
    for kind, mine, count in (("early", my_early, EARLY), ("late", c == 0, chips)):
        finish(kind, mine, count)
        for (q, ih), (where, place) in UNITS.items():
            if where != kind:
                continue
            lanes = pl.ds(128 * ih, 128)
            home = homes[kind]
            if kind == "early":
                first, second = lane_blocks([home[chip] for chip in place])
                out_ref[q, 0:16, lanes] = first
                out_ref[q, 16:32, lanes] = second
            else:
                columns = [divmod(4 * place + h, 3) for h in range(4)]
                for m in range(3):
                    out_ref[q, 8 * m : 8 * m + 8, lanes] = chosen(
                        [(home[chip, 8 * m : 8 * m + 8], i) for chip, i in columns]
                    )
                out_ref[q, 24:32, lanes] = chosen([(home[chip, 8 * i : 8 * i + 8], 3) for chip, i in columns])


def body(f_home, levels, plan):
    chips = lax.axis_size("blocks")
    f32, i32 = jnp.float32, jnp.int32
    dma = pltpu.SemaphoreType.DMA
    out = pl.pallas_call(
        lambda *refs: kernel(chips, *refs),
        out_shape=pltpu.VMEM((19, 32, 512), f32),
        in_specs=[pl.BlockSpec(memory_space=pltpu.HBM)] * 3,
        out_specs=pl.BlockSpec(memory_space=pltpu.VMEM),
        scratch_shapes=[
            pltpu.VMEM((2 * chips, 1, 128), i32),
            pltpu.SMEM((32,), i32),
            pltpu.SMEM((32,), i32),
            pltpu.VMEM((4, 19, 32, 128), f32),
            pltpu.VMEM((19, 4, 32, 128), f32),
            pltpu.VMEM((STEPS, 2, 19, 4, 6, 8, 128), f32),
            pltpu.VMEM((19, 4, 4, 8, 128), f32),
            pltpu.VMEM((STEPS, 2, 5, 4, 8, 128), f32),
            pltpu.VMEM((STEPS, 2, 5, 6, 8, 128), f32),
            pltpu.VMEM((3, 4, 8, 128), f32),
            dma((6,)),
            dma((STEPS, 16)),
            dma((STEPS, 16)),
            dma((4,)),
            dma((4,)),
            pltpu.SemaphoreType.REGULAR((3,)),
        ]
        + [pltpu.VMEM((64, size, 128), f32) for size in (16, 24)]
        + [pltpu.VMEM((64, size, 128), f32) for size in (16, 24)]
        + [pltpu.VMEM((2 * chips, size, 128), f32) for size in (16, 24)]
        + [pltpu.VMEM((64 * chips, 128), f32)] * 2
        + [pltpu.VMEM((48, 32, 128), f32)]
        + [
            pltpu.VMEM((128, 128), i32),
            pltpu.VMEM((128, 128), i32),
            pltpu.SMEM((128, 128), i32),
            dma,
            dma((8,)),
        ],
        compiler_params=pltpu.CompilerParams(
            collective_id=0, has_side_effects=True, vmem_limit_bytes=VMEM_LIMIT
        ),
        name="lattice_and_owners",
    )(f_home.transpose(1, 0, 2), levels, plan)
    return out.transpose(1, 0, 2)


def solution(mesh):
    spec = P(("blocks", "cross"))
    return jax.shard_map(
        body, mesh=mesh, in_specs=(spec, spec, spec), out_specs=spec, check_vma=False
    )
```

```python
import jax
import jax.numpy as jnp
from jax import lax
from jax.experimental import pallas as pl
from jax.experimental.pallas import tpu as pltpu
from jax.sharding import PartitionSpec as P

STEPS = 2
MESH = pl.DeviceIdType.MESH
VELOCITIES = (
    (0, 0, 0),
    (1, 0, 0),
    (-1, 0, 0),
    (0, 1, 0),
    (0, -1, 0),
    (0, 0, 1),
    (0, 0, -1),
    (1, 1, 0),
    (-1, -1, 0),
    (1, -1, 0),
    (-1, 1, 0),
    (1, 0, 1),
    (-1, 0, -1),
    (1, 0, -1),
    (-1, 0, 1),
    (0, 1, 1),
    (0, -1, -1),
    (0, 1, -1),
    (0, -1, 1),
)
WEIGHTS = (1.0 / 3.0,) + (1.0 / 18.0,) * 6 + (1.0 / 36.0,) * 12
PAIRS = tuple((q, q + 1) for q in range(1, 19, 2))
X_SPEEDS = ((1, 7, 9, 11, 13), (2, 8, 10, 12, 14))
Y_SPEEDS = ((3, 7, 10, 15, 17), (4, 8, 9, 16, 18))
TAU_COARSE = 0.55
TAU_FINE = 2.0 * TAU_COARSE - 0.5
RESCALE = TAU_FINE / (2.0 * TAU_COARSE)
INFLOW = 0.08


def row_units():
    early, late = [], []
    for q in range(19):
        for ih in range(4):
            ready = ((1, 2), (2,), (1,))[VELOCITIES[q][0]]
            (early if ih in ready else late).append((q, ih))
    chips = []
    for b in range(64):
        x, z, y = b // 16, b // 4 % 4, b % 4
        if (x + z) % 2 or y != (x + z) % 4:
            chips.append(b)
    units = {}
    for n, row in enumerate(early):
        units[row] = ("early", chips[2 * n : 2 * n + 2])
    for n, row in enumerate(late):
        units[row] = ("late", n)
    return units


UNITS = row_units()
EARLY = 56
VMEM_LIMIT = 56 * 1024 * 1024


def has_early(b):
    diagonal = mod(div(b, 16) + div(b, 4))
    return (lax.rem(diagonal, jnp.int32(2)) == 1) | (mod(b) != diagonal)


def inflow_value(speed):
    along = VELOCITIES[speed][0] * INFLOW
    return WEIGHTS[speed] * (1.0 + 3.0 * along + 4.5 * along * along - 1.5 * INFLOW * INFLOW)


def equilibrium(field):
    density = field[0]
    for q in range(1, 19):
        density = density + field[q]
    inverse = 1.0 / density
    velocity = []
    for axis in range(3):
        total = None
        for q in range(1, 19):
            sign = VELOCITIES[q][axis]
            if sign:
                if total is None:
                    total = field[q] if sign > 0 else -field[q]
                else:
                    total = total + field[q] if sign > 0 else total - field[q]
        velocity.append(total * inverse)
    ux, uy, uz = velocity
    base = 1.0 - 1.5 * (ux * ux + uy * uy + uz * uz)
    out = [None] * 19
    out[0] = WEIGHTS[0] * density * base
    for plus, minus in PAIRS:
        along = None
        for axis in range(3):
            sign = VELOCITIES[plus][axis]
            if sign:
                term = velocity[axis]
                if along is None:
                    along = term
                else:
                    along = along + term if sign > 0 else along - term
        even = base + 4.5 * along * along
        odd = 3.0 * along
        scale = WEIGHTS[plus] * density
        out[plus] = scale * (even + odd)
        out[minus] = scale * (even - odd)
    return out


def lattice_masks(shape):
    lane = lax.broadcasted_iota(jnp.int32, shape, len(shape) - 1)
    return lane, (lane // 8) % 8, lane % 8


def wide_roll(values, shift, axis):
    shift = shift % values.shape[axis]
    return values if shift == 0 else pltpu.roll(values, shift, axis)


def shifted(main, other, q):
    ex, ey, ez = VELOCITIES[q]
    n = main.shape[0]
    lane, j, k = lattice_masks((1, 8, 128))
    if ex > 0:
        main = jnp.where(lane[None] < 64, main, other)
    elif ex < 0:
        main = jnp.where(lane[None] >= 64, main, other)
    turn = 64 if ex else 0
    here = main[:, 1:5].reshape(4 * n, 8, 128)
    if ey > 0:
        there = main[:, 0:4].reshape(4 * n, 8, 128)
        here = jnp.where(j > 0, wide_roll(here, turn + 8, 2), wide_roll(there, turn - 56, 2))
        turn = 0
    elif ey < 0:
        there = main[:, 2:6].reshape(4 * n, 8, 128)
        here = jnp.where(j < 7, wide_roll(here, turn - 8, 2), wide_roll(there, turn + 56, 2))
        turn = 0
    if ez > 0:
        over = wide_roll(wide_roll(here, 1, 1), turn - 7, 2)
        here = jnp.where(k > 0, wide_roll(here, turn + 1, 2), over)
    elif ez < 0:
        over = wide_roll(wide_roll(here, 7, 1), turn + 7, 2)
        here = jnp.where(k < 7, wide_roll(here, turn - 1, 2), over)
    else:
        here = wide_roll(here, turn, 2)
    return here.reshape(n, 4, 8, 128)


def lane_blocks(parts):
    n = len(parts)
    section = lax.broadcasted_iota(jnp.int32, parts[0].shape, parts[0].ndim - 1) // (128 // n)
    out = []
    for h in range(n):
        total = parts[h]
        for m in range(n):
            if m != h:
                total = jnp.where(section == m, wide_roll(parts[m], 128 // n * (m - h), total.ndim - 1), total)
        out.append(total)
    return out


def chosen(parts):
    section = lax.broadcasted_iota(jnp.int32, (8, 128), 1) // 32
    total = None
    for h, (part, at) in enumerate(parts):
        part = wide_roll(part, 32 * (h - at), 1)
        total = part if total is None else jnp.where(section == h, part, total)
    return total


def shifted_inside(work, q, ih):
    ex, ey, ez = VELOCITIES[q]
    lane, j, k = lattice_masks((1, 8, 128))
    main = work[q, ih]
    inside = None

    def both_of(first, second):
        return second if first is None else first & second

    if ex:
        low = lane < 64
        if 0 <= ih - ex < 4:
            main = jnp.where(low if ex > 0 else ~low, main, work[q, ih - ex])
        else:
            inside = ~low if ex > 0 else low
    if ey:
        inside = both_of(inside, (j > 0) if ey > 0 else (j < 7))
    if ez:
        inside = both_of(inside, (k > 0) if ez > 0 else (k < 7))
    return wide_roll(main, (64 if ex else 0) + 8 * ey + ez, 2), inside


def lbm_steps(
    blocks, f_hbm, levels_hbm, plan_hbm, sends, late_rows, plan_all, levels, plan, raw, state, both, work, pack_x, halo_x, coef,
    load_sem, send_sem, recv_sem, round_send, round_recv, ready, send_early,
):
    b = lax.axis_index("blocks")
    c = lax.axis_index("cross")
    has_low, has_high = b > 0, b < blocks - 1
    low, high = jnp.maximum(b - 1, 0), jnp.minimum(b + 1, blocks - 1)

    loads = [
        pltpu.make_async_copy(
            f_hbm.at[:, :, pl.ds(128 * ih, 128)], raw.at[ih], load_sem.at[ih]
        )
        for ih in range(4)
    ]
    numbers = [
        pltpu.make_async_copy(levels_hbm, levels, load_sem.at[4]),
        pltpu.make_async_copy(plan_hbm, plan, load_sem.at[5]),
    ]
    for load in numbers + loads:
        load.start()

    barrier = pltpu.get_barrier_semaphore()

    def greet(device):
        pl.semaphore_signal(barrier, inc=1, device_id=device, device_id_type=MESH)

    greet((b, 1 - c))

    def line(axis):
        stride = (16, 4, 1)[axis]
        at = (b // stride) % 4
        return [b + stride * ((at + k) % 4 - at) for k in (1, 2, 3)]

    for axis in range(3):
        for chip in line(axis):
            greet((chip, c))

    @pl.when(has_low)
    def _():
        greet((low, c))
        greet((low, 1 - c))

    @pl.when(has_high)
    def _():
        greet((high, c))
        greet((high, 1 - c))

    for load in numbers:
        load.wait()
    sublane = lax.broadcasted_iota(jnp.int32, (8, 128), 0)
    for py in range(4):
        fine = jnp.zeros((8, 128), jnp.float32)
        for pz in range(8):
            fine = jnp.where(sublane == pz, levels[py * 8 + pz].astype(jnp.float32), fine)
        is_fine = fine > 0.5
        coef[0, py] = fine
        coef[1, py] = jnp.where(is_fine, (1.0 - 1.0 / TAU_FINE) / RESCALE, 1.0 - 1.0 / TAU_COARSE)
        coef[2, py] = jnp.where(is_fine, 1.0 - 1.0 / TAU_FINE, RESCALE * (1.0 - 1.0 / TAU_COARSE))

    for step in range(STEPS):
        for side in range(2):

            @pl.when(jnp.logical_not(has_low if side == 0 else has_high))
            def _():
                for n, q in enumerate(X_SPEEDS[side]):
                    halo_x[step, side, n] = jnp.full((6, 8, 128), inflow_value(q), jnp.float32)

    plan_row = jnp.zeros((1, 128), jnp.int32)
    plan_lane = lax.broadcasted_iota(jnp.int32, (1, 128), 1)
    for p in range(32):
        plan_row = jnp.where(plan_lane == p, plan[p], plan_row)
    plan_all[64 * c + b] = plan_row

    def plan_round(number):
        size = (1, 4, 16, 64)[number]
        part = plan_all.at[pl.ds(64 * c + (b // size) * size, size)]
        peers = [(b, 1 - c)] if number == 3 else [(chip, c) for chip in line(2 - number)]
        copies = [
            pltpu.make_async_remote_copy(
                src_ref=part,
                dst_ref=part,
                send_sem=round_send.at[number],
                recv_sem=round_recv.at[number],
                device_id=peer,
                device_id_type=MESH,
            )
            for peer in peers
        ]
        for copy in copies:
            copy.start()

    def end_round(number):
        moved = plan_all.at[pl.ds(0, (3, 12, 48, 64)[number])]
        pltpu.make_async_copy(moved, moved, round_recv.at[number]).wait()
        pltpu.make_async_copy(moved, moved, round_send.at[number]).wait()

    for load in loads:
        load.wait()

    lane = lax.broadcasted_iota(jnp.int32, (4, 8, 128), 2)
    pending = []

    def over_outer(body):
        def at(pos, carry):
            body(3 * (pos // 4), pos % 4)
            return carry

        lax.fori_loop(0, 8, at, 0)

    def over_inner(body):
        def at(pos, carry):
            body(1 + pos // 4, pos % 4)
            return carry

        lax.fori_loop(0, 8, at, 0)

    for step in range(STEPS):

        def relax_both(ih, py):
            rows_of_py = pl.ds(pl.multiple_of(py * 8, 8), 8)
            if step:
                field = [state[q, ih, rows_of_py, :] for q in range(19)]
            else:
                field = [raw[ih, q, rows_of_py, :] for q in range(19)]
            balance = equilibrium(field)
            for_coarse, for_fine = coef[1, py], coef[2, py]
            for q in range(19):
                away = field[q] - balance[q]
                both[step, 0, q, ih, py + 1] = balance[q] + for_coarse * away
                both[step, 1, q, ih, py + 1] = balance[q] + for_fine * away

        over_outer(relax_both)

        copies = []

        def add(src, dst, device, send_if, recv_if):
            index = len(copies)
            copy = pltpu.make_async_remote_copy(
                src_ref=src,
                dst_ref=dst,
                send_sem=send_sem.at[step, index],
                recv_sem=recv_sem.at[step, index],
                device_id=device,
                device_id_type=MESH,
            )
            copies.append((send_if, recv_if, copy))

        for side in range(2):
            edge = 3 if side == 0 else 0
            for n, q in enumerate(X_SPEEDS[side]):
                first = both[step, 0, q, edge, 1:5]
                second = pltpu.roll(both[step, 1, q, edge, 1:5], 64, 2)
                keep = lane >= 64 if side == 0 else lane < 64
                pack_x[step, side, n] = jnp.where(keep, first, second)
        if step == 0:
            pl.semaphore_wait(
                barrier, 10 + 2 * has_low.astype(jnp.int32) + 2 * has_high.astype(jnp.int32)
            )
            for chip in line(2):
                pl.semaphore_signal(ready.at[0], inc=1, device_id=(chip, c), device_id_type=MESH)
        for side in range(2):
            target = high if side == 0 else low
            send_if, recv_if = (has_high, has_low) if side == 0 else (has_low, has_high)
            add(
                pack_x.at[step, side],
                halo_x.at[step, side, :, pl.ds(1, 4)],
                (target, c),
                send_if,
                recv_if,
            )
            for n, q in enumerate(X_SPEEDS[side]):
                ey = VELOCITIES[q][1]
                if ey:
                    py, slot = (3, 0) if ey > 0 else (0, 5)
                    add(
                        pack_x.at[step, side, n, py],
                        halo_x.at[step, side, n, slot],
                        (target, 1 - c),
                        send_if,
                        recv_if,
                    )
        def start(chosen):
            for send_if, recv_if, copy in chosen:
                if send_if is None:
                    copy.start()
                else:
                    pl.when(send_if)(copy.start)

        def arrive(chosen):
            for send_if, recv_if, copy in chosen:
                if recv_if is None:
                    copy.wait_recv()
                else:
                    pl.when(recv_if)(copy.wait_recv)

        start(copies)
        along_x = len(copies)
        over_inner(relax_both)
        for side in range(2):
            py, slot = (4, 0) if side == 0 else (1, 5)
            for q in Y_SPEEDS[side]:
                add(
                    both.at[step, :, q, :, py],
                    both.at[step, :, q, :, slot],
                    (b, 1 - c),
                    None,
                    None,
                )
        start(copies[along_x:])
        if step == 0:
            plan_round(0)
        else:
            end_round(1)
            plan_round(2)
        fine = coef[0]

        def stream(q, first, last, halo):
            ex = VELOCITIES[q][0]
            result = []
            for kind in range(2):
                other = None
                if halo:
                    side = 0 if ex > 0 else 1
                    other = halo_x[step, side, X_SPEEDS[side].index(q)]
                    other = (pltpu.roll(other, 64, 2) if kind else other)[None]
                elif ex:
                    other = both[step, kind, q, first - ex : last - ex]
                result.append(shifted(both[step, kind, q, first:last], other, q))
            moved = jnp.where(fine[None] > 0.5, result[1], result[0])
            state[q, first:last] = moved.reshape(last - first, 32, 128)

        arrive(copies[along_x:])
        for q in range(19):
            ex = VELOCITIES[q][0]
            stream(q, 1 if ex > 0 else 0, 3 if ex < 0 else 4, False)

        def relax_again(ih, py):
            rows_of_py = pl.ds(pl.multiple_of(py * 8, 8), 8)
            field = [state[q, ih, rows_of_py, :] for q in range(19)]
            balance = equilibrium(field)
            for q in range(19):
                work[q, ih, py] = field[q] + (1.0 / TAU_FINE) * (balance[q] - field[q])

        def finish(q, ih):
            moved, inside = shifted_inside(work, q, ih)
            inside = fine > 0.5 if inside is None else inside & (fine > 0.5)
            result = jnp.where(inside, moved, state[q, ih].reshape(4, 8, 128)).reshape(32, 128)
            if step == STEPS - 1:
                kind, place = UNITS[q, ih]
                if kind == "late":
                    late_rows[place] = result
                else:
                    for chip, block in zip(place, lane_blocks([result[:16], result[16:]])):
                        sends[kind][chip] = block
            else:
                state[q, ih] = result

        if step == 0:
            pl.semaphore_wait(ready.at[0], 3)
            for chip in line(1):
                pl.semaphore_signal(ready.at[1], inc=1, device_id=(chip, c), device_id_type=MESH)
        over_inner(relax_again)
        last = step == STEPS - 1
        early = [row for row, unit in UNITS.items() if unit[0] == "early"]
        if last:
            for q, ih in early:
                finish(q, ih)
            pl.semaphore_wait(ready.at[2], 1)
            send_early()
        arrive(copies[:along_x])
        pending += copies
        if step == 0:
            end_round(0)
            plan_round(1)
            pl.semaphore_wait(ready.at[1], 3)
            pl.semaphore_signal(ready.at[2], inc=1, device_id=(b, 1 - c), device_id_type=MESH)
        else:
            end_round(2)
            plan_round(3)
        for side in range(2):
            for q in X_SPEEDS[side]:
                stream(q, 3 * side, 3 * side + 1, True)
        over_outer(relax_again)
        for q in range(19):
            for ih in range(4):
                if not (last and (q, ih) in early):
                    finish(q, ih)

    def drain():
        for send_if, recv_if, copy in pending:
            if send_if is None:
                copy.wait_send()
            else:
                pl.when(send_if)(copy.wait_send)

    return drain, lambda: end_round(3)


def mod(value):
    return lax.rem(value, jnp.int32(4))


def div(value, by):
    return lax.div(value, jnp.int32(by))


def chip_beside(b, dx, dz, dy):
    return 16 * mod(div(b, 16) + dx) + 4 * mod(div(b, 4) + dz) + mod(b + dy)


def chip_at(b, k):
    dz = k + div(k, 4)
    return chip_beside(b, k, dz, dz + div(k, 16))


OFFSETS = [
    (k % 4, (k + k // 4) % 4, (k + k // 4 + k // 16) % 4) for k in (*range(63, 0, -1), 0)
]


def migrate(chips, sends, late_rows, plan_all, homes, plan_turned, inv_vec, inv_smem, wide, ordered, outs, local_sem, sems):
    b = lax.axis_index("blocks")
    c = lax.axis_index("cross")
    source = 64 * c + b
    cores = {"early": 1, "late": 0}
    sizes = {"early": 16, "late": 24}

    def remote(src, dst, send, recv, device):
        pltpu.make_async_remote_copy(
            src_ref=src, dst_ref=dst, send_sem=send, recv_sem=recv, device_id=device, device_id_type=MESH
        ).start()

    def wait_for(kind, sem, count):
        part = wide.at[pl.ds(0, sizes[kind] * count)]
        pltpu.make_async_copy(part, part, sems.at[sem]).wait()

    number = {"early": 0, "late": 4}

    def spread(kind, offset):
        chip = chip_beside(b, *offset)

        def send():
            n = number[kind]
            land = wide.at[pl.ds(pl.multiple_of(source * 32, 32), sizes[kind])]
            remote(sends[kind].at[chip], land, sems.at[n], sems.at[n + 1], (chip, cores[kind]))

        if kind == "early":
            wanted = has_early(chip)
            pl.when(wanted if any(offset) else wanted & (c != cores[kind]))(send)
        elif any(offset):
            send()
        else:
            pl.when(c != cores[kind])(send)

    def send_early():
        for offset in OFFSETS:
            spread("early", offset)

    end_plan = yield send_early

    for chip in range(64):
        columns = [divmod(3 * chip + i, 4) for i in range(3)]
        for m in range(3):
            parts = [(late_rows[n, 8 * m : 8 * m + 8], h) for n, h in columns]
            n, h = columns[m]
            sends["late"][chip, 8 * m : 8 * m + 8] = chosen(parts + [(late_rows[n, 24:32], h)])

    for offset in OFFSETS:
        spread("late", offset)
    end_plan()

    plans = plan_all[:, 0, :]
    plan_turned[...] = plans.T
    sub = lax.broadcasted_iota(jnp.int32, (128, 128), 0)
    lane = lax.broadcasted_iota(jnp.int32, (128, 128), 1)

    def place(p, carry):
        plans, total = carry
        owner = plan_turned[pl.ds(p, 1), :] // 32
        hot = jnp.where(owner == sub, 1.0, 0.0)
        slot = plans[:, 0:1] % 32
        value = jnp.where(slot == lane, sub, jnp.where(slot + 32 == lane, p, 0))
        total = total + jnp.dot(
            hot.astype(jnp.bfloat16),
            value.astype(jnp.float32).astype(jnp.bfloat16),
            preferred_element_type=jnp.float32,
        )
        return pltpu.roll(plans, 127, 1), total

    _, total = lax.fori_loop(0, 32, place, (plans, jnp.zeros((128, 128), jnp.float32)), unroll=4)
    total = total.astype(jnp.int32)
    inv_vec[...] = jnp.clip(total * 32 + pltpu.roll(total, 96, 1), 0, 64 * chips - 1)
    move = pltpu.make_async_copy(inv_vec, inv_smem, local_sem)
    move.start()
    move.wait()

    def serve(kind):
        out, size, n = outs[kind], sizes[kind], number[kind]
        core = cores[kind]
        wide[pl.ds(pl.multiple_of(source * 32, 32), size), :] = sends[kind][b]
        wait_for(kind, n + 1, 2 * chips - 1)
        section = lax.broadcasted_iota(jnp.int32, (8, 128), 1) // 32

        def widen(s, carry):
            at = lambda m: pl.ds(pl.multiple_of(s * 32 + 8 * m, 8), 8)
            if kind == "early":
                for m in range(2):
                    wide[at(2 + m), :] = wide_roll(wide[at(m), :], 64, 1)
            else:
                wide[at(3), :] = chosen([(wide[at(m), :], 3) for m in range(3)])
            return carry

        lax.fori_loop(0, 2 * chips, widen, 0, unroll=64)

        def pick(chip, target_core):
            owner = 2 * chip + target_core
            for u in range(32):
                index = inv_smem[owner, u]
                ordered[pl.ds(owner * 32 + u, 1), :] = wide[pl.ds(index, 1), :]
            blocks = [ordered[pl.ds(pl.multiple_of(owner * 32 + 8 * m, 8), 8), :] for m in range(4)]
            if kind == "early":
                for m in range(2):
                    out[owner, 8 * m : 8 * m + 8] = jnp.where(
                        section < 2, blocks[m], wide_roll(blocks[2 + m], 64, 1)
                    )
            else:
                for m in range(3):
                    out[owner, 8 * m : 8 * m + 8] = jnp.where(
                        section < 3, blocks[m], wide_roll(blocks[3], 32 * (3 - m), 1)
                    )

        def send(chip, target_core):
            remote(out.at[2 * chip + target_core], homes[kind].at[b], sems.at[n + 2], sems.at[n + 3], (chip, target_core))

        def step(k, before):
            chip = chip_at(b, chips - k)
            pick(chip, 0)
            pick(chip, 1)

            @pl.when(k > 1)
            def _():
                send(before, 0)
                send(before, 1)

            return chip

        lax.fori_loop(1, chips + 1, step, b)
        homes[kind][b] = out[2 * b + core]
        send(b, 1 - core)

    my_early = (c == 1) & has_early(b)
    pl.when(c == 1)(lambda: wait_for("late", number["late"], chips))
    pl.when(my_early)(lambda: serve("early"))
    pl.when(c == 0)(lambda: serve("late"))

    def finish(kind, mine, count):
        n = number[kind]
        for holds, held in ((True, mine), (False, jnp.logical_not(mine))):

            @pl.when(held)
            def _():
                wait_for(kind, n + 3, count - holds)
                if kind == "early" or holds:
                    wait_for(kind, n, count - holds)
                if holds:
                    wait_for(kind, n + 2, 2 * chips - 1)

    return finish, my_early, c


def kernel(chips, f_hbm, levels, plan, out_ref, *scratch):
    kinds = ("early", "late")
    take = iter(scratch)
    plan_all = next(take)
    lbm = [next(take) for _ in range(15)]
    sends, homes, outs = ({kind: next(take) for kind in kinds} for _ in range(3))
    wide, ordered, late_rows = next(take), next(take), next(take)
    plan_turned, inv_vec, inv_smem, local_sem, sems = take
    moving = migrate(chips, sends, late_rows, plan_all, homes, plan_turned, inv_vec, inv_smem, wide, ordered, outs, local_sem, sems)
    send_early = next(moving)
    drain, end_plan = lbm_steps(chips, f_hbm, levels, plan, sends, late_rows, plan_all, *lbm, send_early)
    try:
        moving.send(end_plan)
    except StopIteration as stop:
        finish, my_early, c = stop.value
    drain()
    for kind, mine, count in (("early", my_early, EARLY), ("late", c == 0, chips)):
        finish(kind, mine, count)
        for (q, ih), (where, place) in UNITS.items():
            if where != kind:
                continue
            lanes = pl.ds(128 * ih, 128)
            home = homes[kind]
            if kind == "early":
                first, second = lane_blocks([home[chip] for chip in place])
                out_ref[q, 0:16, lanes] = first
                out_ref[q, 16:32, lanes] = second
            else:
                columns = [divmod(4 * place + h, 3) for h in range(4)]
                for m in range(3):
                    out_ref[q, 8 * m : 8 * m + 8, lanes] = chosen(
                        [(home[chip, 8 * m : 8 * m + 8], i) for chip, i in columns]
                    )
                out_ref[q, 24:32, lanes] = chosen([(home[chip, 8 * i : 8 * i + 8], 3) for chip, i in columns])


def body(f_home, levels, plan):
    chips = lax.axis_size("blocks")
    f32, i32 = jnp.float32, jnp.int32
    dma = pltpu.SemaphoreType.DMA
    out = pl.pallas_call(
        lambda *refs: kernel(chips, *refs),
        out_shape=pltpu.VMEM((19, 32, 512), f32),
        in_specs=[pl.BlockSpec(memory_space=pltpu.HBM)] * 3,
        out_specs=pl.BlockSpec(memory_space=pltpu.VMEM),
        scratch_shapes=[
            pltpu.VMEM((2 * chips, 1, 128), i32),
            pltpu.SMEM((32,), i32),
            pltpu.SMEM((32,), i32),
            pltpu.VMEM((4, 19, 32, 128), f32),
            pltpu.VMEM((19, 4, 32, 128), f32),
            pltpu.VMEM((STEPS, 2, 19, 4, 6, 8, 128), f32),
            pltpu.VMEM((19, 4, 4, 8, 128), f32),
            pltpu.VMEM((STEPS, 2, 5, 4, 8, 128), f32),
            pltpu.VMEM((STEPS, 2, 5, 6, 8, 128), f32),
            pltpu.VMEM((3, 4, 8, 128), f32),
            dma((6,)),
            dma((STEPS, 16)),
            dma((STEPS, 16)),
            dma((4,)),
            dma((4,)),
            pltpu.SemaphoreType.REGULAR((3,)),
        ]
        + [pltpu.VMEM((64, size, 128), f32) for size in (16, 24)]
        + [pltpu.VMEM((64, size, 128), f32) for size in (16, 24)]
        + [pltpu.VMEM((2 * chips, size, 128), f32) for size in (16, 24)]
        + [pltpu.VMEM((64 * chips, 128), f32)] * 2
        + [pltpu.VMEM((48, 32, 128), f32)]
        + [
            pltpu.VMEM((128, 128), i32),
            pltpu.VMEM((128, 128), i32),
            pltpu.SMEM((128, 128), i32),
            dma,
            dma((8,)),
        ],
        compiler_params=pltpu.CompilerParams(
            collective_id=0, has_side_effects=True, vmem_limit_bytes=VMEM_LIMIT
        ),
        name="lattice_and_owners",
    )(f_home.transpose(1, 0, 2), levels, plan)
    return out.transpose(1, 0, 2)


def solution(mesh):
    spec = P(("blocks", "cross"))
    return jax.shard_map(
        body, mesh=mesh, in_specs=(spec, spec, spec), out_specs=spec, check_vma=False
    )
```
